256 devices in a mesh: img: 32 (over y, x, core), strip: 8 (over z).
Axes of the slice: x: 4, y: 4, z: 8, core: 2. Of those that a mesh axis runs over, the one named last changes fastest.
Arguments:
- image_in: bfloat16 [32, 256, 128, 128], P('img', 'strip'), may hold values from -6 to 6
- cotangent: bfloat16 [32, 256, 128, 128], P('img', 'strip'), may hold values from -6 to 6
- conv1_w: bfloat16 [3, 3, 128, 128], replicated, may hold values from -0.1875 to 0.1875
- conv2_w: bfloat16 [3, 3, 128, 128], replicated, may hold values from -0.1875 to 0.1875
- norm1_gain: float32 [128], replicated, may hold values from 0.5 to 1.5
- norm1_shift: float32 [128], replicated, may hold values from -3 to 3
- norm2_gain: float32 [128], replicated, may hold values from 0.5 to 1.5
- norm2_shift: float32 [128], replicated, may hold values from -3 to 3
- strip_rows: int32 [32, 8], P('img', 'strip'), may hold values from 1 to 32, 128 in all within a row
Outputs:
- image_grad: bfloat16 [32, 256, 128, 128], P('img', 'strip')
- conv1_grad: float32 [1152, 128], P('img')
- conv2_grad: float32 [1152, 128], P('img')
- norm_grads: float32 [4, 128], replicated
The draws below stay inside these ranges and needn't reach their ends.
Inputs may be any that keep to these rules, and one draw needn't show every extreme that they name: `strip_rows`: each image's 8 strip lengths sum to 128; in every image one strip holds exactly 32 rows.
All inputs are finite; a program needn't handle non-finite values. No bound on the sum of `strip_rows` on one device may be relied on, other than what follows from the above.
Results may differ from the reference program's by a relative error of at most 0.0055.
Values may be sent and summed in bfloat16 or wider, within the bound.
No kernel may reach another device: no remote copies, remote signals or barrier semaphores. Data moves between devices by JAX's collectives and lax.ppermute only.
A program may use at most 64 MiB of HBM per device.

```python
import math
import jax
import jax.numpy as jnp
import numpy as np
from jax import lax

C = 128
GROUPS = 32
CAP = 32
COLS = 128
IMAGES = 32
ROWS_ALL = 256
HEIGHT = 128
N_STRIP = 8


def steps_of(rng, extent, pieces, smallest, top_value):
    def one(dim, parts):
        heights = jax.random.uniform(jax.random.fold_in(jax.random.fold_in(rng, 6), dim), (parts,), jnp.float32, smallest / len(pieces), top_value / len(pieces))
        return jnp.repeat(jnp.exp(heights), extent[dim] // parts).reshape((-1,) + (1,) * (len(extent) - dim - 1))

    level = one(*pieces[0])
    for cut in pieces[1:]:
        level = level * one(*cut)
    return level


def split_up(number_of, total, most, skew):
    portions = [(1 << 20) // math.isqrt(grade ** skew) + 1 for grade in range(2, number_of + 1)]
    surplus, counts = total - most - (number_of - 1), [1] * (number_of - 1)
    while surplus > 0:
        movable = [i for i in range(number_of - 1) if counts[i] < most]
        pool, left = sum([portions[i] for i in movable]), surplus
        for i in movable:
            more = min(most - counts[i], max(1, left * portions[i] // pool), surplus)
            counts[i] = counts[i] + more
            surplus = surplus - more
    return np.array([most] + counts)


def uneven_parts(stream_key, number_of, total, bound, skew):
    if number_of == 2:
        one = jax.random.randint(stream_key, (), max(1, total - bound), min(bound, total - 1) + 1)
        return jnp.stack([one, total - one])
    sizes = jnp.asarray(split_up(number_of, total, bound, skew), jnp.int32)
    twos = (number_of - 1) // 2
    source_of, sink = sizes[1:1 + 2 * twos:2], sizes[2:2 + 2 * twos:2]
    margin = jnp.minimum(source_of - 1, bound - sink)
    moved = jax.random.randint(jax.random.fold_in(stream_key, 1), (twos,), 0, 1 << 20) % (margin + 1)
    sizes = sizes.at[1:1 + 2 * twos:2].set(source_of - moved).at[2:2 + 2 * twos:2].set(sink + moved)
    return sizes[jax.random.permutation(jax.random.fold_in(stream_key, 2), number_of)]


def centred(stream_key, extent, deviation, bound, pieces=(), kind=jnp.bfloat16):
    values = deviation * jax.random.normal(stream_key, extent, jnp.float32)
    if pieces:
        values = values * steps_of(stream_key, extent, pieces, -0.22, 0.18)
    return jnp.clip(values, -bound, bound).astype(kind)


def setup_inputs(seed: int = 0) -> dict:
    keys = jax.random.split(jax.random.key(seed), 10)
    return {
        "image_in": centred(keys[0], (IMAGES, ROWS_ALL, COLS, C), 1.0, 6.0, ((0, 32), (1, 8))),
        "cotangent": centred(keys[1], (IMAGES, ROWS_ALL, COLS, C), 1.0, 6.0, ((0, 32), (1, 8))),
        "conv1_w": centred(keys[2], (3, 3, C, C), (9 * C) ** -0.5, 0.1875),
        "conv2_w": centred(keys[3], (3, 3, C, C), (9 * C) ** -0.5, 0.1875),
        "norm1_gain": jnp.clip(1.0 + 0.1 * jax.random.normal(keys[4], (C,), jnp.float32), 0.5, 1.5),
        "norm1_shift": centred(keys[5], (C,), 0.5, 3.0, (), jnp.float32),
        "norm2_gain": jnp.clip(1.0 + 0.1 * jax.random.normal(keys[6], (C,), jnp.float32), 0.5, 1.5),
        "norm2_shift": centred(keys[7], (C,), 0.5, 3.0, (), jnp.float32),
        "strip_rows": jax.vmap(lambda own: uneven_parts(own, N_STRIP, HEIGHT, CAP, 2))(jax.random.split(keys[8], IMAGES)).reshape((IMAGES, N_STRIP)).astype(jnp.int32),
    }


EPSILON = 1e-06

def silu_slope(pre_act):
    logistic = jax.nn.sigmoid(pre_act)
    return logistic * (1.0 + pre_act * (1.0 - logistic))

def group_average(values):
    per_channel = lax.optimization_barrier(jnp.sum(values, axis=(0, 1)))
    grouped = per_channel.reshape(GROUPS, -1)
    return jnp.repeat(lax.optimization_barrier(jnp.sum(grouped, axis=1)) / (values.shape[0] * values.shape[1] * grouped.shape[1]), grouped.shape[1])

def group_norm(values, gain, shift):
    mean_val = group_average(values)
    centered = values - mean_val
    variance = group_average(centered * centered)
    inv_std = lax.rsqrt(variance + EPSILON)
    normed = centered * inv_std
    return (normed, normed * gain + shift, inv_std)

def norm_backward(grad_pre, normed, gain, inv_std):
    scaled = grad_pre * gain
    return inv_std * (scaled - group_average(scaled) - normed * group_average(scaled * normed))

def convolve(padded, kernel, row_count, col_count):
    running = jnp.zeros((row_count * col_count, kernel.shape[3]), jnp.float32)
    for tap_row in range(3):
        for tap_col in range(3):
            window = padded[tap_row:tap_row + row_count, tap_col:tap_col + col_count].reshape(row_count * col_count, -1)
            running = running + jnp.dot(window, kernel[tap_row, tap_col], preferred_element_type=jnp.float32)
    return running.reshape(row_count, col_count, -1)

def kernel_grad(padded, upstream, row_count, col_count):
    flat_up = upstream.reshape(row_count * col_count, -1)
    tap_grads = []
    for tap_row in range(3):
        for tap_col in range(3):
            window = padded[tap_row:tap_row + row_count, tap_col:tap_col + col_count].reshape(row_count * col_count, -1)
            tap_grads.append(lax.dot_general(window, flat_up, (((0,), (0,)), ((), ())), preferred_element_type=jnp.float32))
    return jnp.stack(tap_grads).reshape(-1, flat_up.shape[1])

def spread_back(upstream, kernel, row_count, col_count):
    flat_up = upstream.reshape(row_count * col_count, -1)
    gradient = jnp.zeros((row_count + 2, col_count + 2, kernel.shape[2]), jnp.float32)
    for tap_row in range(3):
        for tap_col in range(3):
            product = lax.dot_general(flat_up, kernel[tap_row, tap_col], (((1,), (1,)), ((), ())), preferred_element_type=jnp.float32)
            product = product.reshape(row_count, col_count, -1)
            gradient = gradient + jnp.pad(product, ((tap_row, 2 - tap_row), (tap_col, 2 - tap_col), (0, 0)))
    return gradient

def compact_index(lengths):
    lengths = lengths.astype(jnp.int32)
    ends = jnp.cumsum(lengths).astype(jnp.int32)
    starts = ends - lengths
    position = jnp.arange(HEIGHT, dtype=jnp.int32)
    owner = lax.optimization_barrier(jnp.sum((position[:, None] >= ends[None, :]).astype(jnp.int32), axis=1)).astype(jnp.int32)
    strip_ids = jnp.arange(N_STRIP, dtype=jnp.int32)
    offset = position - lax.optimization_barrier(jnp.sum(jnp.where(owner[:, None] == strip_ids[None, :], starts[None, :], 0), axis=1)).astype(jnp.int32)
    return (owner * CAP + offset).astype(jnp.int32)

def reference(image_in, cotangent, conv1_w, conv2_w, norm1_gain, norm1_shift, norm2_gain, norm2_shift, strip_rows):

    def one_image(operands):
        source, upstream, lengths = operands
        row_ids = compact_index(lengths)
        inputs = source[row_ids].astype(jnp.float32)
        grad_out = upstream[row_ids]
        normed_one, pre_one, inv_one = group_norm(inputs, norm1_gain, norm1_shift)
        act_one = jax.nn.silu(pre_one).astype(jnp.bfloat16)
        padded_one = jnp.pad(act_one, ((1, 1), (1, 1), (0, 0)))
        hidden = convolve(padded_one, conv1_w, HEIGHT, COLS)
        normed_two, pre_two, inv_two = group_norm(hidden, norm2_gain, norm2_shift)
        act_two = jax.nn.silu(pre_two).astype(jnp.bfloat16)
        padded_two = jnp.pad(act_two, ((1, 1), (1, 1), (0, 0)))
        grad_two = kernel_grad(padded_two, grad_out, HEIGHT, COLS)
        back_two = spread_back(grad_out, conv2_w, HEIGHT, COLS)[1:-1, 1:-1]
        dpre_two = back_two * silu_slope(pre_two)
        hidden_grad = norm_backward(dpre_two, normed_two, norm2_gain, inv_two).astype(jnp.bfloat16)
        grad_one = kernel_grad(padded_one, hidden_grad, HEIGHT, COLS)
        back_one = spread_back(hidden_grad, conv1_w, HEIGHT, COLS)[1:-1, 1:-1]
        dpre_one = back_one * silu_slope(pre_one)
        branch = norm_backward(dpre_one, normed_one, norm1_gain, inv_one)
        result = (grad_out.astype(jnp.float32) + branch).astype(jnp.bfloat16)
        full = jnp.zeros((ROWS_ALL, COLS, C), jnp.bfloat16).at[row_ids].set(result)
        norm_terms = jnp.stack([lax.optimization_barrier(jnp.sum(dpre_one * normed_one, axis=(0, 1))), lax.optimization_barrier(jnp.sum(dpre_one, axis=(0, 1))), lax.optimization_barrier(jnp.sum(dpre_two * normed_two, axis=(0, 1))), lax.optimization_barrier(jnp.sum(dpre_two, axis=(0, 1)))])
        return (full, grad_one, grad_two, norm_terms)
    image_grad, grads_one, grads_two, norm_terms = lax.map(one_image, (image_in, cotangent, strip_rows))
    return (image_grad, lax.optimization_barrier(jnp.sum(grads_one, axis=0)), lax.optimization_barrier(jnp.sum(grads_two, axis=0)), lax.optimization_barrier(jnp.sum(norm_terms, axis=0)))
```

```python
import functools

import jax
import jax.numpy as jnp
from jax import lax
from jax.experimental import pallas as pl
from jax.experimental.pallas import tpu as pltpu
from jax.sharding import Mesh
from jax.sharding import PartitionSpec as P

IMG = ("img_0", "img_1", "img_2")
EPSILON = 1e-06
F32 = jnp.float32
BF16 = jnp.bfloat16
SLOTS = 32
COLS = 128
CH = 128
HEIGHT = 128
PER_GROUP = 4
PEERS = 8
CELLS = float(HEIGHT * COLS * PER_GROUP)
WIDE = 3 * CH
PAIR = 2 * WIDE
MIB = 1 << 20

VMEM = pl.BlockSpec(memory_space=pltpu.VMEM)
SMEM = pl.BlockSpec(memory_space=pltpu.SMEM)
HBM = pl.BlockSpec(memory_space=pltpu.HBM)


def shape(dims, dtype):
    return jax.ShapeDtypeStruct(dims, dtype)


def call(body, in_specs, outs, flops=0, moved=0, scratch=(), limit=12 * MIB, outs_in=None, name=None):
    return pl.pallas_call(
        body,
        in_specs=in_specs,
        out_specs=outs_in or [VMEM] * len(outs),
        out_shape=outs,
        scratch_shapes=scratch,
        compiler_params=pltpu.CompilerParams(vmem_limit_bytes=limit),
        cost_estimate=pl.CostEstimate(flops=flops, bytes_accessed=moved, transcendentals=0),
        name=name,
    )


def folded(row):
    lanes = jnp.broadcast_to(row, (8, CH))
    lane = lax.broadcasted_iota(jnp.int32, (8, CH), 1)
    lanes = lanes + jnp.where(lane % 2 == 0, pltpu.roll(lanes, CH - 1, 1), pltpu.roll(lanes, 1, 1))
    lanes = lanes + jnp.where(lane % 4 < 2, pltpu.roll(lanes, CH - 2, 1), pltpu.roll(lanes, 2, 1))
    return lanes[0:1]


def group_stats(stats):
    total = stats[0, 0:1]
    for j in range(1, PEERS):
        total = total + stats[j, 0:1]
    mean = folded(total) / CELLS
    spread = jnp.zeros((1, CH), F32)
    for j in range(PEERS):
        count = stats[j, 2:3] * float(COLS)
        gap = stats[j, 0:1] / count - mean
        spread = spread + stats[j, 1:2] + count * gap * gap
    return mean, lax.rsqrt(folded(spread) / CELLS + EPSILON)


def moments(sums, gain):
    cross, plain = sums[0, 0:1], sums[0, 1:2]
    for j in range(1, PEERS):
        cross, plain = cross + sums[j, 0:1], plain + sums[j, 1:2]
    return folded(cross * gain) / CELLS, folded(plain * gain) / CELLS


def sums8(value):
    return jnp.sum(value.reshape(-1, 8, value.shape[-1]), axis=0)


def send(out_ref, rows):
    index = lax.broadcasted_iota(jnp.int32, (8, CH), 0)
    tile = jnp.zeros((8, CH), F32)
    for k, row in enumerate(rows):
        tile = jnp.where(index == k, row, tile)
    for j in range(PEERS):
        out_ref[j] = tile


def channel_stats(load, length, out_ref):
    def first(i, acc):
        for k in range(4):
            r = i * 4 + k
            acc = acc + jnp.where(r < length, sums8(load(r)), 0.0)
        return acc

    total = jnp.sum(lax.fori_loop(0, SLOTS // 4, first, jnp.zeros((8, CH), F32)), axis=0, keepdims=True)
    used = length.astype(F32)
    mean = total / (used * float(COLS))

    def second(i, acc):
        for k in range(4):
            r = i * 4 + k
            gap = load(r) - mean
            acc = acc + jnp.where(r < length, sums8(gap * gap), 0.0)
        return acc

    spread = jnp.sum(lax.fori_loop(0, SLOTS // 4, second, jnp.zeros((8, CH), F32)), axis=0, keepdims=True)
    send(out_ref, [total, spread, jnp.broadcast_to(used, (1, CH))])


def sigmoid(z):
    return 0.5 * jnp.tanh(0.5 * z) + 0.5


def taps(row):
    col = lax.broadcasted_iota(jnp.int32, (COLS, CH), 0)
    before = jnp.where(col == 0, 0.0, pltpu.roll(row, 1, 0))
    after = jnp.where(col == COLS - 1, 0.0, pltpu.roll(row, COLS - 1, 0))
    return jnp.concatenate([before.astype(BF16), row.astype(BF16), after.astype(BF16)], axis=1)


def place_halo(buf, length, above, below):
    buf[0, :, 0:WIDE] = above[0]
    buf[0, :, WIDE:PAIR] = above[1]
    pair = (length + 2) // 2

    @pl.when(length % 2 == 0)
    def _():
        buf[pair, :, 0:WIDE] = below[0]
        buf[pair, :, WIDE:PAIR] = below[1]

    @pl.when(length % 2 == 1)
    def _():
        buf[pair, :, WIDE:PAIR] = below[0]
        buf[pair + 1, :, 0:WIDE] = below[1]


def convolve(buf, w_ref, pairs, chunk, store):
    for begin in range(0, pairs, chunk):
        count = min(chunk, pairs - begin)
        upper = buf[begin : begin + count].reshape(count * COLS, PAIR)
        lower = buf[begin + 1 : begin + 1 + count].reshape(count * COLS, PAIR)
        out = jnp.dot(upper, w_ref[0], preferred_element_type=F32)
        out = out + jnp.dot(lower, w_ref[1], preferred_element_type=F32)
        store(begin, count, out.reshape(count, COLS, 2 * CH))


def row_weight(h, length, ends):
    own = jnp.where((h >= 1) & (h <= length), 1.0, 0.0)
    return jnp.where(h == 0, ends[0], jnp.where(h == length + 1, ends[1], own))


def row_ends(stats, strip, length):
    start, _, _ = lengths_around(stats, strip)
    return jnp.minimum(start, 1.0), jnp.where(start + length.astype(F32) <= HEIGHT - 1.0, 1.0, 0.0)


def lengths_around(stats, strip):
    start = jnp.zeros((1, CH), F32)
    above = jnp.zeros((1, CH), F32)
    below = jnp.zeros((1, CH), F32)
    for j in range(PEERS):
        here = stats[j, 2:3]
        start = start + jnp.where(j < strip, here, 0.0)
        above = above + jnp.where(j == strip - 1, here, 0.0)
        below = below + jnp.where(j == strip + 1, here, 0.0)
    return start, above, below


def transposed_taps(load, length, out_ref):
    def step(p, carry):
        for k in range(2):
            tile = load(p, k).astype(F32).T.astype(BF16)
            for tap in range(3):
                o = 2 * p + k - 1 - tap
                parity = (k - 1 - tap) % 2
                q = p + (k - 1 - tap - parity) // 2
                kept = jnp.where((o >= 0) & (o < length), tile, jnp.zeros_like(tile))
                lanes = pl.multiple_of((q + 2) * COLS, COLS)
                out_ref[parity, tap * CH : (tap + 1) * CH, pl.ds(lanes, COLS)] = kept
        return carry

    lax.fori_loop(0, SLOTS // 2 + 2, step, 0)


def kernel_grad(rows_t, even, odd):
    used = slice(2 * COLS, 2 * COLS + SLOTS // 2 * COLS)
    grad = jnp.dot(rows_t[0, :, used], even.reshape(-1, WIDE), preferred_element_type=F32)
    return grad + jnp.dot(rows_t[1, :, used], odd.reshape(-1, WIDE), preferred_element_type=F32)


def stats_kernel(len_ref, x_ref, g_ref, top_ref, bottom_ref, top2_ref, bottom2_ref, out_ref, rows_ref, sem, edge_sem):
    length = len_ref[0, 0]
    last = length - 1
    near = jnp.maximum(length - 2, 0)
    whole = pltpu.make_async_copy(x_ref, rows_ref, sem)
    whole.start()
    copies = []
    for k, (ref, row) in enumerate(((x_ref, 0), (g_ref, 0), (x_ref, 1), (g_ref, 1))):
        copies.append((ref.at[row], top_ref.at[k]))
    for k, (ref, row) in enumerate(((x_ref, last), (g_ref, last), (x_ref, near), (g_ref, near))):
        copies.append((ref.at[row], bottom_ref.at[k]))
    for k, ref in enumerate((x_ref, g_ref)):
        copies.append((ref.at[0], top2_ref.at[k]))
        copies.append((ref.at[last], bottom2_ref.at[k]))
    started = [pltpu.make_async_copy(a, b, edge_sem.at[i]) for i, (a, b) in enumerate(copies)]
    for copy in started:
        copy.start()
    whole.wait()
    channel_stats(lambda r: rows_ref[r].astype(F32), length, out_ref)
    for copy in started:
        copy.wait()


def weights_kernel(first_ref, second_ref, ahead_ref, turned1_ref, turned2_ref):
    for out_ref in (ahead_ref, turned1_ref, turned2_ref):
        out_ref[0, WIDE * 0 : WIDE, CH : 2 * CH] = jnp.zeros((WIDE, CH), BF16)
        out_ref[1, WIDE:PAIR, 0:CH] = jnp.zeros((WIDE, CH), BF16)
    for a in range(3):
        for b in range(3):
            for v in range(2):
                half, lane = divmod((a + v) * WIDE + b * CH, PAIR)
                ahead_ref[half, lane : lane + CH, v * CH : (v + 1) * CH] = first_ref[a, b]
            for w_ref, out_ref in ((first_ref, turned1_ref), (second_ref, turned2_ref)):
                tile = w_ref[2 - a, 2 - b].astype(F32).T.astype(BF16)
                for v in range(2):
                    half, lane = divmod((a + v) * WIDE + b * CH, PAIR)
                    out_ref[half, lane : lane + CH, v * CH : (v + 1) * CH] = tile


def hidden_kernel(
    len_ref, strip_ref, x_ref, up_ref, down_ref, up2_ref, down2_ref, st_ref, w_ref, gain_ref, shift_ref,
    hid_ref, act_ref, out_ref,
):
    length, strip = len_ref[0, 0], strip_ref[0]
    mean, inv = group_stats(st_ref)
    scale, shift = inv * gain_ref[...], shift_ref[...]
    start, above, below = lengths_around(st_ref, strip)

    def act(row):
        pre = (row.astype(F32) - mean) * scale + shift
        return pre * sigmoid(pre)

    act_ref[SLOTS // 2 + 1] = jnp.zeros((COLS, PAIR), BF16)

    def step(p, carry):
        act_ref[p + 1, :, 0:WIDE] = taps(act(x_ref[2 * p]))
        act_ref[p + 1, :, WIDE:PAIR] = taps(act(x_ref[2 * p + 1]))
        return carry

    lax.fori_loop(0, SLOTS // 2, step, 0)
    end = start + length.astype(F32)
    far_up = jnp.where(above >= 2.0, up_ref[2].astype(F32), up2_ref[0].astype(F32))
    far_down = jnp.where(below >= 2.0, down_ref[2].astype(F32), down2_ref[0].astype(F32))
    place_halo(
        act_ref,
        length,
        [
            taps(jnp.where(start >= 2.0, act(far_up), 0.0)),
            taps(jnp.where(start >= 1.0, act(up_ref[0]), 0.0)),
        ],
        [
            taps(jnp.where(end <= HEIGHT - 1.0, act(down_ref[0]), 0.0)),
            taps(jnp.where(end <= HEIGHT - 2.0, act(far_down), 0.0)),
        ],
    )

    def store(begin, count, out):
        for k in range(count):
            hid_ref[2 * (begin + k)] = out[k, :, 0:CH]
            hid_ref[2 * (begin + k) + 1] = out[k, :, CH:]

    convolve(act_ref, w_ref, SLOTS // 2 + 1, 6, store)
    channel_stats(lambda r: hid_ref[r + 1], length, out_ref)


def back_kernel(
    len_ref, strip_ref, g_ref, up_ref, down_ref, up2_ref, down2_ref, st_ref, w_ref, act_ref,
    g_taps_ref, back_ref, act_t_ref,
):
    length, strip = len_ref[0, 0], strip_ref[0]
    _, above, below = lengths_around(st_ref, strip)
    g_taps_ref[SLOTS // 2 + 1] = jnp.zeros((COLS, PAIR), BF16)

    def step(p, carry):
        g_taps_ref[p + 1, :, 0:WIDE] = taps(g_ref[2 * p].astype(F32))
        g_taps_ref[p + 1, :, WIDE:PAIR] = taps(g_ref[2 * p + 1].astype(F32))
        return carry

    lax.fori_loop(0, SLOTS // 2, step, 0)
    far_up = jnp.where(above >= 2.0, up_ref[3].astype(F32), up2_ref[1].astype(F32))
    far_down = jnp.where(below >= 2.0, down_ref[3].astype(F32), down2_ref[1].astype(F32))
    place_halo(
        g_taps_ref,
        length,
        [taps(far_up), taps(up_ref[1].astype(F32))],
        [taps(down_ref[1].astype(F32)), taps(far_down)],
    )

    def store(begin, count, out):
        for k in range(count):
            back_ref[2 * (begin + k)] = out[k, :, 0:CH]
            back_ref[2 * (begin + k) + 1] = out[k, :, CH:]

    convolve(g_taps_ref, w_ref, SLOTS // 2 + 1, 6, store)
    transposed_taps(lambda p, k: act_ref[p, :, k * WIDE + CH : k * WIDE + 2 * CH], length, act_t_ref)


def dpre2_kernel(len_ref, strip_ref, st1_ref, st_ref, hid_ref, back_ref, gain_ref, shift_ref, act_ref, dpre_ref, out_ref):
    length = len_ref[0, 0]
    ends = row_ends(st1_ref, strip_ref[0], length)
    mean, inv = group_stats(st_ref)
    gain, shift = gain_ref[...], shift_ref[...]

    def step(i, carry):
        cross, plain = carry
        for k in range(2):
            h = 2 * i + k
            normed = (hid_ref[h] - mean) * inv
            pre = normed * gain + shift
            s = sigmoid(pre)
            act = pre * s
            grad = back_ref[h] * (s + act * (1.0 - s))
            own = (h >= 1) & (h <= length)
            inside = row_weight(h, length, ends) > 0.5
            act_ref[h] = jnp.where(inside, act, 0.0).astype(BF16)
            grad = jnp.where(inside, grad, 0.0)
            dpre_ref[h] = grad
            mine = jnp.where(own, grad, 0.0)
            plain = plain + sums8(mine)
            cross = cross + sums8(jnp.where(own, grad * normed, 0.0))
        return cross, plain

    zero = jnp.zeros((8, CH), F32)
    cross, plain = lax.fori_loop(0, SLOTS // 2 + 1, step, (zero, zero))
    send(out_ref, [jnp.sum(cross, axis=0, keepdims=True), jnp.sum(plain, axis=0, keepdims=True)])


def grad2_kernel(len_ref, act_ref, g_taps_ref, out_ref, act_t_ref):
    length = len_ref[0, 0]

    def load(p, k):
        row = jnp.clip(2 * p + k - 1, 0, SLOTS + 1)
        return act_ref[row]

    transposed_taps(load, length, act_t_ref)
    half = SLOTS // 2
    out_ref[...] = kernel_grad(
        act_t_ref, g_taps_ref[1 : half + 1, :, 0:WIDE], g_taps_ref[1 : half + 1, :, WIDE:PAIR]
    )


def dpre1_kernel(
    len_ref, strip_ref, st1_ref, st2_ref, sums_ref, own_sums_ref, hid_ref, dpre2_ref, act_t_ref, x_ref, grad2_ref, w_ref,
    gain1_ref, shift1_ref, gain2_ref,
    share_ref, dpre_ref, out_ref, d_taps_ref, grad1_ref,
):
    length = len_ref[0, 0]
    ends = row_ends(st1_ref, strip_ref[0], length)
    half = SLOTS // 2
    mean2, inv2 = group_stats(st2_ref)
    gain2 = gain2_ref[...]
    cross2, plain2 = moments(sums_ref, gain2)

    def step(i, carry):
        for k in range(2):
            h = 2 * i + k
            normed = (hid_ref[h] - mean2) * inv2
            grad = inv2 * (dpre2_ref[h] * gain2 - plain2 - normed * cross2)
            inside = row_weight(h, length, ends) > 0.5
            d_taps_ref[i, :, k * WIDE : (k + 1) * WIDE] = taps(jnp.where(inside, grad, 0.0))
        return carry

    lax.fori_loop(0, half + 1, step, 0)
    grad1_ref[...] = kernel_grad(act_t_ref, d_taps_ref[0:half, :, WIDE:PAIR], d_taps_ref[1 : half + 1, :, 0:WIDE])

    def store(begin, count, out):
        for k in range(count):
            dpre_ref[2 * (begin + k)] = out[k, :, 0:CH]
            dpre_ref[2 * (begin + k) + 1] = out[k, :, CH:]

    convolve(d_taps_ref, w_ref, half, 8, store)
    mean1, inv1 = group_stats(st1_ref)
    gain1, shift1 = gain1_ref[...], shift1_ref[...]

    def slope(i, carry):
        cross, plain = carry
        for k in range(2):
            r = 2 * i + k
            normed = (x_ref[r].astype(F32) - mean1) * inv1
            pre = normed * gain1 + shift1
            s = sigmoid(pre)
            grad = jnp.where(r < length, dpre_ref[r] * (s + pre * s * (1.0 - s)), 0.0)
            dpre_ref[r] = grad
            plain = plain + sums8(grad)
            cross = cross + sums8(grad * normed)
        return cross, plain

    zero = jnp.zeros((8, CH), F32)
    cross, plain = lax.fori_loop(0, half, slope, (zero, zero))
    cross, plain = jnp.sum(cross, axis=0, keepdims=True), jnp.sum(plain, axis=0, keepdims=True)
    index = lax.broadcasted_iota(jnp.int32, (8, CH), 0)
    norm = jnp.where(index == 0, cross, jnp.where(index == 1, plain, 0.0))
    out_ref[...] = norm
    norm = norm + jnp.where(index == 2, own_sums_ref[0, 0:1], 0.0) + jnp.where(index == 3, own_sums_ref[0, 1:2], 0.0)
    blocks, rows = share_ref.shape[0], (share_ref.shape[1] - 8) // 2
    for j in range(blocks):
        share_ref[j] = packed(cut(grad1_ref, j * rows, rows), cut(grad2_ref, j * rows, rows), norm)


def cut(ref, begin, count):
    pieces = []
    while count:
        tap, row = divmod(begin, CH)
        here = min(count, CH - row)
        a, b = divmod(tap, 3)
        pieces.append(ref[a * CH + row : a * CH + row + here, (2 - b) * CH : (3 - b) * CH])
        begin, count = begin + here, count - here
    return pieces


def packed(first, second, norm):
    high = norm.astype(BF16).astype(F32)
    return jnp.concatenate([*first, *second, high[0:4], (norm - high)[0:4]], axis=0).astype(BF16)


def unpacked(total):
    rows = (total.shape[0] - 8) // 2
    norm = total[2 * rows : 2 * rows + 4] + total[2 * rows + 4 :]
    return total[0:rows], total[rows : 2 * rows], norm


def relay_kernel(in_ref, own_ref, out_ref):
    total = in_ref[0].astype(F32)
    for j in range(1, in_ref.shape[0]):
        total = total + in_ref[j].astype(F32)
    first, second, norm = unpacked(total)
    norm = jnp.concatenate([norm, jnp.zeros((4, CH), F32)], axis=0)
    own = own_ref[...]
    high = own.astype(BF16).astype(F32)
    image = jnp.concatenate([high[0:4], (own - high)[0:4]], axis=0).astype(BF16)
    tile = jnp.concatenate([packed([first], [second], norm), image], axis=0)
    for j in range(PEERS):
        out_ref[j] = tile


def finish_kernel(
    len_ref, in_ref, st_ref, x_ref, g_ref, dpre_ref, gain_ref, image_ref, first_ref, second_ref, norm_ref
):
    total = in_ref[0].astype(F32)
    for j in range(1, PEERS):
        total = total + in_ref[j].astype(F32)
    rows = first_ref.shape[0]
    first_ref[...], second_ref[...], norm_ref[...] = unpacked(total[0 : 2 * rows + 8])
    sums = total[2 * rows + 8 : 2 * rows + 12] + total[2 * rows + 12 : 2 * rows + 16]
    length = len_ref[0, 0]
    mean, inv = group_stats(st_ref)
    gain = gain_ref[...]
    cross, plain = folded(sums[0:1] * gain) / CELLS, folded(sums[1:2] * gain) / CELLS

    def step(i, carry):
        for k in range(2):
            r = 2 * i + k
            normed = (x_ref[r].astype(F32) - mean) * inv
            grad = inv * (dpre_ref[r] * gain - plain - normed * cross)
            grad = jnp.where(r < length, g_ref[r].astype(F32) + grad, 0.0)
            image_ref[r] = grad.astype(BF16)
        return carry

    lax.fori_loop(0, SLOTS // 2, step, 0)


def exchanged(value, axis):
    return lax.all_to_all(value, axis, split_axis=0, concat_axis=0, tiled=True)


def shifted(value, by):
    count = PEERS
    pairs = [(i, i + by) for i in range(count) if 0 <= i + by < count]
    return lax.ppermute(value, "strip", pairs)


def body(
    image_in, cotangent, conv1_w, conv2_w, norm1_gain, norm1_shift, norm2_gain, norm2_shift, strip_rows
):
    x, g = image_in[0], cotangent[0]
    gain1, shift1 = norm1_gain[None], norm1_shift[None]
    gain2, shift2 = norm2_gain[None], norm2_shift[None]
    strip = lax.axis_index("strip")
    strip_id = strip.reshape(1).astype(jnp.int32)
    images = lax.axis_size(IMG)
    half = SLOTS // 2
    field = SLOTS * COLS * CH
    conv_flops = 2 * 9 * field * CH
    edge = (COLS, CH)
    stat = shape((PEERS, 8, CH), F32)

    top, bottom, top2, bottom2, stats1 = call(
        stats_kernel,
        [SMEM, HBM, HBM],
        [shape((4, *edge), BF16), shape((4, *edge), BF16), shape((2, *edge), BF16), shape((2, *edge), BF16), stat],
        flops=field * 6,
        moved=field * 2,
        scratch=[pltpu.VMEM((SLOTS, *edge), BF16), pltpu.SemaphoreType.DMA, pltpu.SemaphoreType.DMA((12,))],
        limit=63 * MIB + MIB // 2,
        name="stats",
    )(strip_rows, x, g)
    up, down = shifted(bottom, 1), shifted(top, -1)
    up2, down2 = shifted(bottom2, 2), shifted(top2, -2)
    weights1, turned1, turned2 = call(
        weights_kernel, [VMEM, VMEM], [shape((2, PAIR, 2 * CH), BF16)] * 3, flops=field * 2, moved=field, name="weights"
    )(conv1_w, conv2_w)
    stats1 = exchanged(stats1, "strip")

    hidden, act1, stats2 = call(
        hidden_kernel,
        [SMEM, SMEM] + [VMEM] * 9,
        [shape((SLOTS + 2, *edge), F32), shape((half + 2, COLS, PAIR), BF16), stat],
        flops=conv_flops,
        moved=field * 6,
        name="hidden",
    )(strip_rows, strip_id, x, up, down, up2, down2, stats1, weights1, gain1, shift1)

    g_taps, back2, act1_t = call(
        back_kernel,
        [SMEM, SMEM] + [VMEM] * 8,
        [
            shape((half + 2, COLS, PAIR), BF16),
            shape((SLOTS + 2, *edge), F32),
            shape((2, WIDE, (half + 4) * COLS), BF16),
        ],
        flops=conv_flops,
        moved=field * 6,
        name="back",
    )(strip_rows, strip_id, g, up, down, up2, down2, stats1, turned2, act1)
    stats2, g_taps, back2, act1_t = lax.optimization_barrier((stats2, g_taps, back2, act1_t))
    stats2 = exchanged(stats2, "strip")

    act2, dpre2, own_sums2 = call(
        dpre2_kernel,
        [SMEM, SMEM] + [VMEM] * 6,
        [shape((SLOTS + 2, *edge), BF16), shape((SLOTS + 2, *edge), F32), stat],
        flops=field * 40,
        moved=field * 8,
        name="dpre2",
    )(strip_rows, strip_id, stats1, stats2, hidden, back2, gain2, shift2)

    (grad2,) = call(
        grad2_kernel,
        [SMEM] + [VMEM] * 2,
        [shape((WIDE, WIDE), F32)],
        flops=conv_flops,
        moved=field * 6,
        scratch=[pltpu.VMEM((2, WIDE, (half + 4) * COLS), BF16)],
        name="grad2",
    )(strip_rows, act2, g_taps)
    own_sums2, grad2 = lax.optimization_barrier((own_sums2, grad2))
    sums2 = exchanged(own_sums2, "strip")

    rows = 9 * CH // images
    share, dpre1, own_sums1 = call(
        dpre1_kernel,
        [SMEM, SMEM] + [VMEM] * 13,
        [shape((images, 2 * rows + 8, CH), BF16), shape((SLOTS, *edge), F32), shape((8, CH), F32)],
        flops=2 * conv_flops,
        moved=field * 8,
        scratch=[pltpu.VMEM((half + 1, COLS, PAIR), BF16), pltpu.VMEM((WIDE, WIDE), F32)],
        name="dpre1",
    )(
        strip_rows, strip_id, stats1, stats2, sums2, own_sums2, hidden, dpre2, act1_t, x, grad2, turned1, gain1, shift1,
        gain2,
    )
    share, dpre1, own_sums1 = lax.optimization_barrier((share, dpre1, own_sums1))
    share = exchanged(share, IMG)
    (relayed,) = call(
        relay_kernel,
        [VMEM, VMEM],
        [shape((PEERS, 2 * rows + 16, CH), BF16)],
        moved=images * (2 * rows + 8) * CH * 2,
        name="relay",
    )(share, own_sums1)
    relayed = exchanged(relayed, "strip")
    image_grad, grad1, grad2, norm_grads = call(
        finish_kernel,
        [SMEM] + [VMEM] * 6,
        [shape((SLOTS, *edge), BF16), shape((rows, CH), F32), shape((rows, CH), F32), shape((4, CH), F32)],
        flops=field * 12,
        moved=field * 10,
        name="finish",
    )(strip_rows, relayed, stats1, x, g, dpre1, gain1)
    return image_grad[None], grad1, grad2, norm_grads


def solution(mesh):
    torus = Mesh(mesh.devices.reshape(4, 4, 2, mesh.shape["strip"]), (*IMG, "strip"))
    return jax.shard_map(
        body,
        mesh=torus,
        in_specs=(
            P(IMG, "strip", None, None), P(IMG, "strip", None, None), P(), P(), P(), P(), P(), P(), P(IMG, "strip"),
        ),
        out_specs=(P(IMG, "strip", None, None), P(IMG, None), P(IMG, None), P()),
        check_vma=False,
    )
```

```python
import jax
import jax.numpy as jnp
from jax import lax
from jax.experimental import pallas as pl
from jax.experimental.pallas import tpu as pltpu
from jax.sharding import Mesh
from jax.sharding import PartitionSpec as P


IMG = ("img_0", "img_1", "img_2")
EPSILON = 1e-06
F32 = jnp.float32
BF16 = jnp.bfloat16
SLOTS = 32
COLS = 128
CH = 128
HEIGHT = 128
PER_GROUP = 4
PEERS = 8
CELLS = float(HEIGHT * COLS * PER_GROUP)
WIDE = 3 * CH
PAIR = 2 * WIDE
MIB = 1 << 20

VMEM = pl.BlockSpec(memory_space=pltpu.VMEM)
SMEM = pl.BlockSpec(memory_space=pltpu.SMEM)
HBM = pl.BlockSpec(memory_space=pltpu.HBM)


def shape(dims, dtype):
    return jax.ShapeDtypeStruct(dims, dtype)


def call(body, in_specs, outs, flops=0, moved=0, scratch=(), limit=12 * MIB, outs_in=None):
    return pl.pallas_call(
        body,
        in_specs=in_specs,
        out_specs=outs_in or [VMEM] * len(outs),
        out_shape=outs,
        scratch_shapes=scratch,
        compiler_params=pltpu.CompilerParams(vmem_limit_bytes=limit),
        cost_estimate=pl.CostEstimate(flops=flops, bytes_accessed=moved, transcendentals=0),
    )


def folded(row):
    lanes = jnp.broadcast_to(row, (8, CH))
    lane = lax.broadcasted_iota(jnp.int32, (8, CH), 1)
    lanes = lanes + jnp.where(lane % 2 == 0, pltpu.roll(lanes, CH - 1, 1), pltpu.roll(lanes, 1, 1))
    lanes = lanes + jnp.where(lane % 4 < 2, pltpu.roll(lanes, CH - 2, 1), pltpu.roll(lanes, 2, 1))
    return lanes[0:1]


def group_stats(stats):
    total = stats[0, 0:1]
    for j in range(1, PEERS):
        total = total + stats[j, 0:1]
    mean = folded(total) / CELLS
    spread = jnp.zeros((1, CH), F32)
    for j in range(PEERS):
        count = stats[j, 2:3] * float(COLS)
        gap = stats[j, 0:1] / count - mean
        spread = spread + stats[j, 1:2] + count * gap * gap
    return mean, lax.rsqrt(folded(spread) / CELLS + EPSILON)


def moments(sums, gain):
    cross, plain = sums[0, 0:1], sums[0, 1:2]
    for j in range(1, PEERS):
        cross, plain = cross + sums[j, 0:1], plain + sums[j, 1:2]
    return folded(cross * gain) / CELLS, folded(plain * gain) / CELLS


def sums8(value):
    return jnp.sum(value.reshape(-1, 8, value.shape[-1]), axis=0)


def send(out_ref, rows):
    index = lax.broadcasted_iota(jnp.int32, (8, CH), 0)
    tile = jnp.zeros((8, CH), F32)
    for k, row in enumerate(rows):
        tile = jnp.where(index == k, row, tile)
    for j in range(PEERS):
        out_ref[j] = tile


def channel_stats(load, length, out_ref):
    def first(i, acc):
        for k in range(4):
            r = i * 4 + k
            acc = acc + jnp.where(r < length, sums8(load(r)), 0.0)
        return acc

    total = jnp.sum(lax.fori_loop(0, SLOTS // 4, first, jnp.zeros((8, CH), F32)), axis=0, keepdims=True)
    used = length.astype(F32)
    mean = total / (used * float(COLS))

    def second(i, acc):
        for k in range(4):
            r = i * 4 + k
            gap = load(r) - mean
            acc = acc + jnp.where(r < length, sums8(gap * gap), 0.0)
        return acc

    spread = jnp.sum(lax.fori_loop(0, SLOTS // 4, second, jnp.zeros((8, CH), F32)), axis=0, keepdims=True)
    send(out_ref, [total, spread, jnp.broadcast_to(used, (1, CH))])


def sigmoid(z):
    return 0.5 * jnp.tanh(0.5 * z) + 0.5


def taps(row):
    col = lax.broadcasted_iota(jnp.int32, (COLS, CH), 0)
    before = jnp.where(col == 0, 0.0, pltpu.roll(row, 1, 0))
    after = jnp.where(col == COLS - 1, 0.0, pltpu.roll(row, COLS - 1, 0))
    return jnp.concatenate([before.astype(BF16), row.astype(BF16), after.astype(BF16)], axis=1)


def place_halo(buf, length, above, below):
    buf[0, :, 0:WIDE] = above
    pair = (length + 1) // 2

    @pl.when(length % 2 == 1)
    def _():
        buf[pair, :, 0:WIDE] = below

    @pl.when(length % 2 == 0)
    def _():
        buf[pair, :, WIDE:PAIR] = below


def fill_taps(buf, load):
    half = SLOTS // 2
    buf[half, :, WIDE:PAIR] = jnp.zeros((COLS, WIDE), BF16)

    def step(p, carry):
        buf[p, :, WIDE:PAIR] = taps(load(2 * p))
        buf[p + 1, :, 0:WIDE] = taps(load(2 * p + 1))
        return carry

    lax.fori_loop(0, half, step, 0)


def convolve(buf, w_ref, out_ref, chunk=8):
    for begin in range(0, SLOTS // 2, chunk):
        upper = buf[begin : begin + chunk].reshape(chunk * COLS, PAIR)
        lower = buf[begin + 1 : begin + 1 + chunk].reshape(chunk * COLS, PAIR)
        out = jnp.dot(upper, w_ref[0], preferred_element_type=F32)
        out = out + jnp.dot(lower, w_ref[1], preferred_element_type=F32)
        out = out.reshape(chunk, COLS, 2 * CH)
        for k in range(chunk):
            out_ref[2 * (begin + k)] = out[k, :, 0:CH]
            out_ref[2 * (begin + k) + 1] = out[k, :, CH:]


def transposed_taps(load, count, ahead, keep, out_ref):
    def step(p, carry):
        for k in range(2):
            i = 2 * p + k
            tile = load(p, k).T
            for tap in range(3):
                parity = (k + ahead - tap) % 2
                q = p + (k + ahead - tap - parity) // 2
                kept = jnp.where(keep(i, i + ahead - tap), tile, jnp.zeros_like(tile))
                lanes = pl.multiple_of((q + 1) * COLS, COLS)
                out_ref[parity, tap * CH : (tap + 1) * CH, pl.ds(lanes, COLS)] = kept
        return carry

    lax.fori_loop(0, count // 2, step, 0)


def kernel_grad(rows_t, even, odd):
    used = slice(COLS, COLS + even.shape[0] * COLS)
    grad = jnp.dot(rows_t[0, :, used], even.reshape(-1, WIDE), preferred_element_type=F32)
    return grad + jnp.dot(rows_t[1, :, used], odd.reshape(-1, WIDE), preferred_element_type=F32)


def stats_kernel(len_ref, x_ref, g_ref, top_ref, bottom_ref, out_ref, rows_ref, sem, edge_sem):
    length = len_ref[0, 0]
    last = length - 1
    whole = pltpu.make_async_copy(x_ref, rows_ref, sem)
    whole.start()
    started = []
    for k, ref in enumerate((x_ref, g_ref)):
        started.append(pltpu.make_async_copy(ref.at[0], top_ref.at[k], edge_sem.at[2 * k]))
        started.append(pltpu.make_async_copy(ref.at[last], bottom_ref.at[k], edge_sem.at[2 * k + 1]))
    for copy in started:
        copy.start()
    whole.wait()
    channel_stats(lambda r: rows_ref[r].astype(F32), length, out_ref)
    for copy in started:
        copy.wait()


def weights_kernel(first_ref, second_ref, ahead_ref, turned1_ref, turned2_ref):
    for out_ref in (ahead_ref, turned1_ref, turned2_ref):
        out_ref[0, WIDE * 0 : WIDE, CH : 2 * CH] = jnp.zeros((WIDE, CH), BF16)
        out_ref[1, WIDE:PAIR, 0:CH] = jnp.zeros((WIDE, CH), BF16)
    for a in range(3):
        for b in range(3):
            for v in range(2):
                half, lane = divmod((a + v) * WIDE + b * CH, PAIR)
                ahead_ref[half, lane : lane + CH, v * CH : (v + 1) * CH] = first_ref[a, b]
            for w_ref, out_ref in ((first_ref, turned1_ref), (second_ref, turned2_ref)):
                tile = w_ref[2 - a, 2 - b].T
                for v in range(2):
                    half, lane = divmod((a + v) * WIDE + b * CH, PAIR)
                    out_ref[half, lane : lane + CH, v * CH : (v + 1) * CH] = tile


def hidden_kernel(
    len_ref, strip_ref, x_ref, up_ref, down_ref, st_ref, w_ref, gain_ref, shift_ref, hid_ref, act_ref, out_ref
):
    length, strip = len_ref[0, 0], strip_ref[0]
    mean, inv = group_stats(st_ref)
    scale, shift = inv * gain_ref[...], shift_ref[...]

    def act(row):
        pre = (row.astype(F32) - mean) * scale + shift
        return pre * sigmoid(pre)

    fill_taps(act_ref, lambda r: act(x_ref[r]))
    place_halo(
        act_ref,
        length,
        taps(jnp.where(strip > 0, act(up_ref[0]), 0.0)),
        taps(jnp.where(strip < PEERS - 1, act(down_ref[0]), 0.0)),
    )
    convolve(act_ref, w_ref, hid_ref)
    channel_stats(lambda r: hid_ref[r], length, out_ref)


def back_kernel(len_ref, strip_ref, g_ref, up_ref, down_ref, w_ref, act_ref, g_taps_ref, back_ref, act_t_ref):
    length, strip = len_ref[0, 0], strip_ref[0]
    fill_taps(g_taps_ref, lambda r: g_ref[r].astype(F32))
    place_halo(
        g_taps_ref,
        length,
        taps(jnp.where(strip > 0, up_ref[1].astype(F32), 0.0)),
        taps(jnp.where(strip < PEERS - 1, down_ref[1].astype(F32), 0.0)),
    )
    convolve(g_taps_ref, w_ref, back_ref)
    transposed_taps(
        lambda p, k: act_ref[p, :, k * WIDE + CH : k * WIDE + 2 * CH],
        SLOTS + 2,
        0,
        lambda i, o: (o >= 0) & (o < length),
        act_t_ref,
    )


def dpre2_kernel(
    len_ref, st_ref, hid_ref, back_ref, gain_ref, shift_ref, act_ref, dpre_ref, top_ref, bottom_ref, out_ref
):
    length = len_ref[0, 0]
    mean, inv = group_stats(st_ref)
    gain, shift = gain_ref[...], shift_ref[...]

    def step(i, carry):
        cross, plain = carry
        for k in range(2):
            r = 2 * i + k
            normed = (hid_ref[r] - mean) * inv
            pre = normed * gain + shift
            s = sigmoid(pre)
            act = pre * s
            act_ref[r] = act.astype(BF16)
            grad = jnp.where(r < length, back_ref[r] * (s + act * (1.0 - s)), 0.0)
            dpre_ref[r] = grad
            plain = plain + sums8(grad)
            cross = cross + sums8(grad * normed)
        return cross, plain

    zero = jnp.zeros((8, CH), F32)
    cross, plain = lax.fori_loop(0, SLOTS // 2, step, (zero, zero))
    send(out_ref, [jnp.sum(cross, axis=0, keepdims=True), jnp.sum(plain, axis=0, keepdims=True)])
    for ref, row in ((top_ref, 0), (bottom_ref, length - 1)):
        ref[0] = dpre_ref[row]
        ref[1] = hid_ref[row]


def grad2_kernel(len_ref, act_ref, g_taps_ref, out_ref, act_t_ref):
    length = len_ref[0, 0]
    half = SLOTS // 2
    for tap, o in ((0, 0), (0, 1), (1, 0), (1, SLOTS + 1), (2, SLOTS), (2, SLOTS + 1)):
        lanes = (o // 2 + 1) * COLS
        act_t_ref[o % 2, tap * CH : (tap + 1) * CH, lanes : lanes + COLS] = jnp.zeros((CH, COLS), BF16)
    transposed_taps(lambda p, k: act_ref[2 * p + k], SLOTS, 2, lambda i, o: i < length, act_t_ref)
    out_ref[...] = kernel_grad(
        act_t_ref, g_taps_ref[0 : half + 1, :, 0:WIDE], g_taps_ref[0 : half + 1, :, WIDE:PAIR]
    )


def dpre1_kernel(
    len_ref, strip_ref, st1_ref, st2_ref, sums_ref, own_sums_ref, hid_ref, dpre2_ref, up_ref, down_ref, act_t_ref,
    x_ref, grad2_ref, w_ref, gain1_ref, shift1_ref, gain2_ref,
    share_ref, dpre_ref, out_ref, d_taps_ref, grad1_ref,
):
    length, strip = len_ref[0, 0], strip_ref[0]
    half = SLOTS // 2
    mean2, inv2 = group_stats(st2_ref)
    gain2 = gain2_ref[...]
    cross2, plain2 = moments(sums_ref, gain2)

    def dhidden(dpre, hidden):
        return inv2 * (dpre * gain2 - plain2 - (hidden - mean2) * inv2 * cross2)

    fill_taps(d_taps_ref, lambda r: jnp.where(r < length, dhidden(dpre2_ref[r], hid_ref[r]), 0.0))
    place_halo(
        d_taps_ref,
        length,
        taps(jnp.where(strip > 0, dhidden(up_ref[0], up_ref[1]), 0.0)),
        taps(jnp.where(strip < PEERS - 1, dhidden(down_ref[0], down_ref[1]), 0.0)),
    )
    grad1_ref[...] = kernel_grad(act_t_ref, d_taps_ref[0:half, :, WIDE:PAIR], d_taps_ref[1 : half + 1, :, 0:WIDE])
    convolve(d_taps_ref, w_ref, dpre_ref)
    mean1, inv1 = group_stats(st1_ref)
    gain1, shift1 = gain1_ref[...], shift1_ref[...]

    def slope(i, carry):
        cross, plain = carry
        for k in range(2):
            r = 2 * i + k
            normed = (x_ref[r].astype(F32) - mean1) * inv1
            pre = normed * gain1 + shift1
            s = sigmoid(pre)
            grad = jnp.where(r < length, dpre_ref[r] * (s + pre * s * (1.0 - s)), 0.0)
            dpre_ref[r] = grad
            plain = plain + sums8(grad)
            cross = cross + sums8(grad * normed)
        return cross, plain

    zero = jnp.zeros((8, CH), F32)
    cross, plain = lax.fori_loop(0, half, slope, (zero, zero))
    cross, plain = jnp.sum(cross, axis=0, keepdims=True), jnp.sum(plain, axis=0, keepdims=True)
    index = lax.broadcasted_iota(jnp.int32, (8, CH), 0)
    norm = jnp.where(index == 0, cross, jnp.where(index == 1, plain, 0.0))
    out_ref[...] = norm
    norm = norm + jnp.where(index == 2, own_sums_ref[0, 0:1], 0.0) + jnp.where(index == 3, own_sums_ref[0, 1:2], 0.0)
    blocks, rows = share_ref.shape[0], (share_ref.shape[1] - 8) // 2
    for j in range(blocks):
        share_ref[j] = packed(cut(grad1_ref, j * rows, rows), cut(grad2_ref, j * rows, rows), norm)


def cut(ref, begin, count):
    pieces = []
    while count:
        tap, row = divmod(begin, CH)
        here = min(count, CH - row)
        a, b = divmod(tap, 3)
        pieces.append(ref[a * CH + row : a * CH + row + here, (2 - b) * CH : (3 - b) * CH])
        begin, count = begin + here, count - here
    return pieces


def packed(first, second, norm):
    high = norm.astype(BF16).astype(F32)
    return jnp.concatenate([*first, *second, high[0:4], (norm - high)[0:4]], axis=0).astype(BF16)


def unpacked(total):
    rows = (total.shape[0] - 8) // 2
    norm = total[2 * rows : 2 * rows + 4] + total[2 * rows + 4 :]
    return total[0:rows], total[rows : 2 * rows], norm


def relay_kernel(in_ref, own_ref, out_ref):
    total = in_ref[0].astype(F32)
    for j in range(1, in_ref.shape[0]):
        total = total + in_ref[j].astype(F32)
    first, second, norm = unpacked(total)
    norm = jnp.concatenate([norm, jnp.zeros((4, CH), F32)], axis=0)
    own = own_ref[...]
    high = own.astype(BF16).astype(F32)
    image = jnp.concatenate([high[0:4], (own - high)[0:4]], axis=0).astype(BF16)
    tile = jnp.concatenate([packed([first], [second], norm), image], axis=0)
    for j in range(PEERS):
        out_ref[j] = tile


def finish_kernel(
    len_ref, in_ref, st_ref, x_ref, g_ref, dpre_ref, gain_ref, image_ref, first_ref, second_ref, norm_ref
):
    total = in_ref[0].astype(F32)
    for j in range(1, PEERS):
        total = total + in_ref[j].astype(F32)
    rows = first_ref.shape[0]
    first_ref[...], second_ref[...], norm_ref[...] = unpacked(total[0 : 2 * rows + 8])
    sums = total[2 * rows + 8 : 2 * rows + 12] + total[2 * rows + 12 : 2 * rows + 16]
    length = len_ref[0, 0]
    mean, inv = group_stats(st_ref)
    gain = gain_ref[...]
    cross, plain = folded(sums[0:1] * gain) / CELLS, folded(sums[1:2] * gain) / CELLS

    def step(i, carry):
        for k in range(2):
            r = 2 * i + k
            normed = (x_ref[r].astype(F32) - mean) * inv
            grad = inv * (dpre_ref[r] * gain - plain - normed * cross)
            grad = jnp.where(r < length, g_ref[r].astype(F32) + grad, 0.0)
            image_ref[r] = grad.astype(BF16)
        return carry

    lax.fori_loop(0, SLOTS // 2, step, 0)


def exchanged(value, axis):
    return lax.all_to_all(value, axis, split_axis=0, concat_axis=0, tiled=True)


def shifted(value, by):
    return lax.ppermute(value, "strip", [(i, (i + by) % PEERS) for i in range(PEERS)])


def body(
    image_in, cotangent, conv1_w, conv2_w, norm1_gain, norm1_shift, norm2_gain, norm2_shift, strip_rows
):
    x, g = image_in[0], cotangent[0]
    gain1, shift1 = norm1_gain[None], norm1_shift[None]
    gain2, shift2 = norm2_gain[None], norm2_shift[None]
    strip = lax.axis_index("strip")
    strip_id = strip.reshape(1).astype(jnp.int32)
    images = lax.axis_size(IMG)
    half = SLOTS // 2
    field = SLOTS * COLS * CH
    conv_flops = 2 * 9 * field * CH
    edge = (COLS, CH)
    stat = shape((PEERS, 8, CH), F32)

    top, bottom, stats1 = call(
        stats_kernel,
        [SMEM, HBM, HBM],
        [shape((2, *edge), BF16), shape((2, *edge), BF16), stat],
        flops=field * 6,
        moved=field * 2,
        scratch=[pltpu.VMEM((SLOTS, *edge), BF16), pltpu.SemaphoreType.DMA, pltpu.SemaphoreType.DMA((4,))],
        limit=63 * MIB + MIB // 2,
    )(strip_rows, x, g)
    up, down = shifted(bottom, 1), shifted(top, -1)
    weights1, turned1, turned2 = call(
        weights_kernel, [VMEM, VMEM], [shape((2, PAIR, 2 * CH), BF16)] * 3, flops=field * 2, moved=field
    )(conv1_w, conv2_w)
    stats1 = exchanged(stats1, "strip")

    hidden, act1, stats2 = call(
        hidden_kernel,
        [SMEM, SMEM] + [VMEM] * 7,
        [shape((SLOTS, *edge), F32), shape((half + 1, COLS, PAIR), BF16), stat],
        flops=conv_flops,
        moved=field * 6,
    )(strip_rows, strip_id, x, up, down, stats1, weights1, gain1, shift1)

    g_taps, back2, act1_t = call(
        back_kernel,
        [SMEM, SMEM] + [VMEM] * 5,
        [
            shape((half + 1, COLS, PAIR), BF16),
            shape((SLOTS, *edge), F32),
            shape((2, WIDE, (half + 2) * COLS), BF16),
        ],
        flops=conv_flops,
        moved=field * 6,
    )(strip_rows, strip_id, g, up, down, turned2, act1)
    stats2, g_taps, back2, act1_t = lax.optimization_barrier((stats2, g_taps, back2, act1_t))
    stats2 = exchanged(stats2, "strip")

    act2, dpre2, top, bottom, own_sums2 = call(
        dpre2_kernel,
        [SMEM] + [VMEM] * 5,
        [
            shape((SLOTS, *edge), BF16), shape((SLOTS, *edge), F32), shape((2, *edge), F32), shape((2, *edge), F32), stat,
        ],
        flops=field * 40,
        moved=field * 8,
    )(strip_rows, stats2, hidden, back2, gain2, shift2)
    up, down = shifted(bottom, 1), shifted(top, -1)

    (grad2,) = call(
        grad2_kernel,
        [SMEM] + [VMEM] * 2,
        [shape((WIDE, WIDE), F32)],
        flops=conv_flops,
        moved=field * 6,
        scratch=[pltpu.VMEM((2, WIDE, (half + 2) * COLS), BF16)],
    )(strip_rows, act2, g_taps)
    own_sums2, grad2, up, down = lax.optimization_barrier((own_sums2, grad2, up, down))
    sums2 = exchanged(own_sums2, "strip")

    rows = 9 * CH // images
    share, dpre1, own_sums1 = call(
        dpre1_kernel,
        [SMEM, SMEM] + [VMEM] * 15,
        [shape((images, 2 * rows + 8, CH), BF16), shape((SLOTS, *edge), F32), shape((8, CH), F32)],
        flops=2 * conv_flops,
        moved=field * 8,
        scratch=[pltpu.VMEM((half + 1, COLS, PAIR), BF16), pltpu.VMEM((WIDE, WIDE), F32)],
    )(
        strip_rows, strip_id, stats1, stats2, sums2, own_sums2, hidden, dpre2, up, down, act1_t, x, grad2, turned1,
        gain1, shift1, gain2,
    )
    share, dpre1, own_sums1 = lax.optimization_barrier((share, dpre1, own_sums1))
    share = exchanged(share, IMG)
    (relayed,) = call(
        relay_kernel, [VMEM, VMEM], [shape((PEERS, 2 * rows + 16, CH), BF16)], moved=images * (2 * rows + 8) * CH * 2
    )(share, own_sums1)
    relayed = exchanged(relayed, "strip")
    image_grad, grad1, grad2, norm_grads = call(
        finish_kernel,
        [SMEM] + [VMEM] * 6,
        [shape((SLOTS, *edge), BF16), shape((rows, CH), F32), shape((rows, CH), F32), shape((4, CH), F32)],
        flops=field * 12,
        moved=field * 10,
    )(strip_rows, relayed, stats1, x, g, dpre1, gain1)
    return image_grad[None], grad1, grad2, norm_grads


def solution(mesh):
    torus = Mesh(mesh.devices.reshape(4, 4, 2, mesh.shape["strip"]), (*IMG, "strip"))
    return jax.shard_map(
        body,
        mesh=torus,
        in_specs=(
            P(IMG, "strip", None, None), P(IMG, "strip", None, None), P(), P(), P(), P(), P(), P(), P(IMG, "strip"),
        ),
        out_specs=(P(IMG, "strip", None, None), P(IMG, None), P(IMG, None), P()),
        check_vma=False,
    )
```

```python
import jax
import jax.numpy as jnp
from jax import lax
from jax.experimental import pallas as pl
from jax.experimental.pallas import tpu as pltpu
from jax.sharding import Mesh
from jax.sharding import PartitionSpec as P


IMG = ("img_0", "img_1", "img_2")
EPSILON = 1e-06
F32 = jnp.float32
BF16 = jnp.bfloat16
SLOTS = 32
COLS = 128
CH = 128
HEIGHT = 128
PER_GROUP = 4
PEERS = 8
CELLS = float(HEIGHT * COLS * PER_GROUP)
WIDE = 3 * CH
PAIR = 2 * WIDE
MIB = 1 << 20

VMEM = pl.BlockSpec(memory_space=pltpu.VMEM)
SMEM = pl.BlockSpec(memory_space=pltpu.SMEM)
HBM = pl.BlockSpec(memory_space=pltpu.HBM)


def shape(dims, dtype):
    return jax.ShapeDtypeStruct(dims, dtype)


def call(body, in_specs, outs, flops=0, moved=0, scratch=(), limit=12 * MIB, outs_in=None):
    return pl.pallas_call(
        body,
        in_specs=in_specs,
        out_specs=outs_in or [VMEM] * len(outs),
        out_shape=outs,
        scratch_shapes=scratch,
        compiler_params=pltpu.CompilerParams(vmem_limit_bytes=limit),
        cost_estimate=pl.CostEstimate(flops=flops, bytes_accessed=moved, transcendentals=0),
    )


def folded(row):
    lanes = jnp.broadcast_to(row, (8, CH))
    lane = lax.broadcasted_iota(jnp.int32, (8, CH), 1)
    lanes = lanes + jnp.where(lane % 2 == 0, pltpu.roll(lanes, CH - 1, 1), pltpu.roll(lanes, 1, 1))
    lanes = lanes + jnp.where(lane % 4 < 2, pltpu.roll(lanes, CH - 2, 1), pltpu.roll(lanes, 2, 1))
    return lanes[0:1]


def group_stats(stats):
    total = stats[0, 0:1]
    for j in range(1, PEERS):
        total = total + stats[j, 0:1]
    mean = folded(total) / CELLS
    spread = jnp.zeros((1, CH), F32)
    for j in range(PEERS):
        count = stats[j, 2:3] * float(COLS)
        gap = stats[j, 0:1] / count - mean
        spread = spread + stats[j, 1:2] + count * gap * gap
    return mean, lax.rsqrt(folded(spread) / CELLS + EPSILON)


def moments(sums, gain):
    cross, plain = sums[0, 0:1], sums[0, 1:2]
    for j in range(1, PEERS):
        cross, plain = cross + sums[j, 0:1], plain + sums[j, 1:2]
    return folded(cross * gain) / CELLS, folded(plain * gain) / CELLS


def sums8(value):
    return jnp.sum(value.reshape(-1, 8, value.shape[-1]), axis=0)


def send(out_ref, rows):
    index = lax.broadcasted_iota(jnp.int32, (8, CH), 0)
    tile = jnp.zeros((8, CH), F32)
    for k, row in enumerate(rows):
        tile = jnp.where(index == k, row, tile)
    for j in range(PEERS):
        out_ref[j] = tile


def channel_stats(load, length, out_ref):
    def first(i, acc):
        for k in range(4):
            r = i * 4 + k
            acc = acc + jnp.where(r < length, sums8(load(r)), 0.0)
        return acc

    total = jnp.sum(lax.fori_loop(0, SLOTS // 4, first, jnp.zeros((8, CH), F32)), axis=0, keepdims=True)
    used = length.astype(F32)
    mean = total / (used * float(COLS))

    def second(i, acc):
        for k in range(4):
            r = i * 4 + k
            gap = load(r) - mean
            acc = acc + jnp.where(r < length, sums8(gap * gap), 0.0)
        return acc

    spread = jnp.sum(lax.fori_loop(0, SLOTS // 4, second, jnp.zeros((8, CH), F32)), axis=0, keepdims=True)
    send(out_ref, [total, spread, jnp.broadcast_to(used, (1, CH))])


def sigmoid(z):
    return 0.5 * jnp.tanh(0.5 * z) + 0.5


def taps(row):
    col = lax.broadcasted_iota(jnp.int32, (COLS, CH), 0)
    before = jnp.where(col == 0, 0.0, pltpu.roll(row, 1, 0))
    after = jnp.where(col == COLS - 1, 0.0, pltpu.roll(row, COLS - 1, 0))
    return jnp.concatenate([before.astype(BF16), row.astype(BF16), after.astype(BF16)], axis=1)


def convolve(buf, w_ref, row_at, finish, beside=lambda step: None, chunk=4):
    built = 0
    for begin in range(0, SLOTS // 2, chunk):
        needed = 2 * (begin + chunk) + 2
        for t in range(built, needed):
            buf[t // 2, :, t % 2 * WIDE : (t % 2 + 1) * WIDE] = taps(row_at(t))
        built = needed
        beside(begin // chunk)
        upper = buf[begin : begin + chunk].reshape(chunk * COLS, PAIR)
        lower = buf[begin + 1 : begin + 1 + chunk].reshape(chunk * COLS, PAIR)
        out = jnp.dot(upper, w_ref[0], preferred_element_type=F32)
        out = out + jnp.dot(lower, w_ref[1], preferred_element_type=F32)
        out = out.reshape(chunk, COLS, 2 * CH)
        for k in range(chunk):
            finish(2 * (begin + k), out[k, :, 0:CH])
            finish(2 * (begin + k) + 1, out[k, :, CH:])


def around(own, up, down, length, t):
    if t == 0:
        return up
    if t == SLOTS + 1:
        return down
    return jnp.where(t <= length, own(t - 1), down)


def in_image(length, strip, t):
    if t == 0:
        return strip > 0
    return (t <= length) | (strip < PEERS - 1)


def transposed_row(tile, i, ahead, keep, out_ref):
    tile = tile.T
    for tap in range(3):
        o = i + ahead - tap
        lanes = (o // 2 + 1) * COLS
        kept = jnp.where(keep(o), tile, jnp.zeros_like(tile))
        out_ref[o % 2, tap * CH : (tap + 1) * CH, lanes : lanes + COLS] = kept


def kernel_grad(rows_t, even, odd):
    used = slice(COLS, COLS + even.shape[0] * COLS)
    grad = jnp.dot(rows_t[0, :, used], even.reshape(-1, WIDE), preferred_element_type=F32)
    return grad + jnp.dot(rows_t[1, :, used], odd.reshape(-1, WIDE), preferred_element_type=F32)


def stats_kernel(len_ref, x_ref, g_ref, top_ref, bottom_ref, out_ref, rows_ref, sem, edge_sem):
    length = len_ref[0, 0]
    last = length - 1
    whole = pltpu.make_async_copy(x_ref, rows_ref, sem)
    whole.start()
    started = []
    for k, ref in enumerate((x_ref, g_ref)):
        started.append(pltpu.make_async_copy(ref.at[0], top_ref.at[k], edge_sem.at[2 * k]))
        started.append(pltpu.make_async_copy(ref.at[last], bottom_ref.at[k], edge_sem.at[2 * k + 1]))
    for copy in started:
        copy.start()
    whole.wait()
    channel_stats(lambda r: rows_ref[r].astype(F32), length, out_ref)
    for copy in started:
        copy.wait()


def weights_kernel(first_ref, second_ref, ahead_ref, turned1_ref, turned2_ref):
    for out_ref in (ahead_ref, turned1_ref, turned2_ref):
        out_ref[0, WIDE * 0 : WIDE, CH : 2 * CH] = jnp.zeros((WIDE, CH), BF16)
        out_ref[1, WIDE:PAIR, 0:CH] = jnp.zeros((WIDE, CH), BF16)
    for a in range(3):
        for b in range(3):
            for v in range(2):
                half, lane = divmod((a + v) * WIDE + b * CH, PAIR)
                ahead_ref[half, lane : lane + CH, v * CH : (v + 1) * CH] = first_ref[a, b]
            for w_ref, out_ref in ((first_ref, turned1_ref), (second_ref, turned2_ref)):
                tile = w_ref[2 - a, 2 - b].T
                for v in range(2):
                    half, lane = divmod((a + v) * WIDE + b * CH, PAIR)
                    out_ref[half, lane : lane + CH, v * CH : (v + 1) * CH] = tile


def hidden_kernel(
    len_ref, strip_ref, x_ref, up_ref, down_ref, st_ref, w_ref, gain_ref, shift_ref, hid_ref, act_ref, out_ref
):
    length, strip = len_ref[0, 0], strip_ref[0]
    mean, inv = group_stats(st_ref)
    scale, shift = inv * gain_ref[...], shift_ref[...]

    def row_at(t):
        row = around(lambda r: x_ref[r], up_ref[0], down_ref[0], length, t)
        pre = (row.astype(F32) - mean) * scale + shift
        return jnp.where(in_image(length, strip, t), pre * sigmoid(pre), 0.0)

    def finish(r, row):
        hid_ref[r] = row

    convolve(act_ref, w_ref, row_at, finish)
    channel_stats(lambda r: hid_ref[r], length, out_ref)


def back_kernel(len_ref, strip_ref, g_ref, up_ref, down_ref, w_ref, act_ref, g_taps_ref, back_ref, act_t_ref):
    length, strip = len_ref[0, 0], strip_ref[0]

    def row_at(t):
        row = around(lambda r: g_ref[r], up_ref[1], down_ref[1], length, t)
        return jnp.where(in_image(length, strip, t), row.astype(F32), 0.0)

    def finish(r, row):
        back_ref[r] = row

    def beside(step):
        for i in range(step * 9, min(step * 9 + 9, SLOTS + 2)):
            tile = act_ref[i // 2, :, i % 2 * WIDE + CH : i % 2 * WIDE + 2 * CH]
            transposed_row(tile, i, 0, lambda o: (o >= 0) & (o < length), act_t_ref)

    convolve(g_taps_ref, w_ref, row_at, finish, beside)


def dpre2_kernel(
    len_ref, st_ref, hid_ref, back_ref, gain_ref, shift_ref, act_ref, dpre_ref, top_ref, bottom_ref, out_ref
):
    length = len_ref[0, 0]
    mean, inv = group_stats(st_ref)
    gain, shift = gain_ref[...], shift_ref[...]

    def step(i, carry):
        cross, plain = carry
        for k in range(2):
            r = 2 * i + k
            normed = (hid_ref[r] - mean) * inv
            pre = normed * gain + shift
            s = sigmoid(pre)
            act = pre * s
            act_ref[r] = act.astype(BF16)
            grad = jnp.where(r < length, back_ref[r] * (s + act * (1.0 - s)), 0.0)
            dpre_ref[r] = grad
            plain = plain + sums8(grad)
            cross = cross + sums8(grad * normed)
        return cross, plain

    zero = jnp.zeros((8, CH), F32)
    cross, plain = lax.fori_loop(0, SLOTS // 2, step, (zero, zero))
    send(out_ref, [jnp.sum(cross, axis=0, keepdims=True), jnp.sum(plain, axis=0, keepdims=True)])
    for ref, row in ((top_ref, 0), (bottom_ref, length - 1)):
        ref[0] = dpre_ref[row]
        ref[1] = hid_ref[row]


def grad2_kernel(len_ref, act_ref, g_taps_ref, out_ref, act_t_ref):
    length = len_ref[0, 0]
    half = SLOTS // 2
    for tap, o in ((0, 0), (0, 1), (1, 0), (1, SLOTS + 1), (2, SLOTS), (2, SLOTS + 1)):
        lanes = (o // 2 + 1) * COLS
        act_t_ref[o % 2, tap * CH : (tap + 1) * CH, lanes : lanes + COLS] = jnp.zeros((CH, COLS), BF16)
    for i in range(SLOTS):
        transposed_row(act_ref[i], i, 2, lambda o: i < length, act_t_ref)
    out_ref[...] = kernel_grad(
        act_t_ref, g_taps_ref[0 : half + 1, :, 0:WIDE], g_taps_ref[0 : half + 1, :, WIDE:PAIR]
    )


def dpre1_kernel(
    len_ref, strip_ref, st1_ref, st2_ref, sums_ref, own_sums_ref, hid_ref, dpre2_ref, up_ref, down_ref, act_t_ref,
    x_ref, grad2_ref, w_ref, gain1_ref, shift1_ref, gain2_ref,
    share_ref, dpre_ref, out_ref, d_taps_ref, grad1_ref,
):
    length, strip = len_ref[0, 0], strip_ref[0]
    half = SLOTS // 2
    mean2, inv2 = group_stats(st2_ref)
    gain2 = gain2_ref[...]
    cross2, plain2 = moments(sums_ref, gain2)

    def dhidden(dpre, hidden):
        return inv2 * (dpre * gain2 - plain2 - (hidden - mean2) * inv2 * cross2)

    mean1, inv1 = group_stats(st1_ref)
    gain1, shift1 = gain1_ref[...], shift1_ref[...]
    sums = [jnp.zeros((8, CH), F32), jnp.zeros((8, CH), F32)]

    def row_at(t):
        dpre = around(lambda r: dpre2_ref[r], up_ref[0], down_ref[0], length, t)
        hidden = around(lambda r: hid_ref[r], up_ref[1], down_ref[1], length, t)
        return jnp.where(in_image(length, strip, t), dhidden(dpre, hidden), 0.0)

    def finish(r, row):
        normed = (x_ref[r].astype(F32) - mean1) * inv1
        pre = normed * gain1 + shift1
        s = sigmoid(pre)
        grad = jnp.where(r < length, row * (s + pre * s * (1.0 - s)), 0.0)
        dpre_ref[r] = grad
        sums[0] = sums[0] + sums8(grad * normed)
        sums[1] = sums[1] + sums8(grad)

    convolve(d_taps_ref, w_ref, row_at, finish)
    grad1_ref[...] = kernel_grad(act_t_ref, d_taps_ref[0:half, :, WIDE:PAIR], d_taps_ref[1 : half + 1, :, 0:WIDE])
    cross, plain = (jnp.sum(total, axis=0, keepdims=True) for total in sums)
    index = lax.broadcasted_iota(jnp.int32, (8, CH), 0)
    norm = jnp.where(index == 0, cross, jnp.where(index == 1, plain, 0.0))
    out_ref[...] = norm
    norm = norm + jnp.where(index == 2, own_sums_ref[0, 0:1], 0.0) + jnp.where(index == 3, own_sums_ref[0, 1:2], 0.0)
    blocks, rows = share_ref.shape[0], (share_ref.shape[1] - 8) // 2
    for j in range(blocks):
        share_ref[j] = packed(cut(grad1_ref, j * rows, rows), cut(grad2_ref, j * rows, rows), norm)


def cut(ref, begin, count):
    pieces = []
    while count:
        tap, row = divmod(begin, CH)
        here = min(count, CH - row)
        a, b = divmod(tap, 3)
        pieces.append(ref[a * CH + row : a * CH + row + here, (2 - b) * CH : (3 - b) * CH])
        begin, count = begin + here, count - here
    return pieces


def packed(first, second, norm):
    high = norm.astype(BF16).astype(F32)
    return jnp.concatenate([*first, *second, high[0:4], (norm - high)[0:4]], axis=0).astype(BF16)


def unpacked(total):
    rows = (total.shape[0] - 8) // 2
    norm = total[2 * rows : 2 * rows + 4] + total[2 * rows + 4 :]
    return total[0:rows], total[rows : 2 * rows], norm


def relay_kernel(in_ref, own_ref, out_ref):
    total = in_ref[0].astype(F32)
    for j in range(1, in_ref.shape[0]):
        total = total + in_ref[j].astype(F32)
    first, second, norm = unpacked(total)
    norm = jnp.concatenate([norm, jnp.zeros((4, CH), F32)], axis=0)
    own = own_ref[...]
    high = own.astype(BF16).astype(F32)
    image = jnp.concatenate([high[0:4], (own - high)[0:4]], axis=0).astype(BF16)
    tile = jnp.concatenate([packed([first], [second], norm), image], axis=0)
    for j in range(PEERS):
        out_ref[j] = tile


def finish_kernel(
    len_ref, in_ref, st_ref, x_ref, g_ref, dpre_ref, gain_ref, image_ref, first_ref, second_ref, norm_ref
):
    total = in_ref[0].astype(F32)
    for j in range(1, PEERS):
        total = total + in_ref[j].astype(F32)
    rows = first_ref.shape[0]
    first_ref[...], second_ref[...], norm_ref[...] = unpacked(total[0 : 2 * rows + 8])
    sums = total[2 * rows + 8 : 2 * rows + 12] + total[2 * rows + 12 : 2 * rows + 16]
    length = len_ref[0, 0]
    mean, inv = group_stats(st_ref)
    gain = gain_ref[...]
    cross, plain = folded(sums[0:1] * gain) / CELLS, folded(sums[1:2] * gain) / CELLS

    def step(i, carry):
        for k in range(2):
            r = 2 * i + k
            normed = (x_ref[r].astype(F32) - mean) * inv
            grad = inv * (dpre_ref[r] * gain - plain - normed * cross)
            grad = jnp.where(r < length, g_ref[r].astype(F32) + grad, 0.0)
            image_ref[r] = grad.astype(BF16)
        return carry

    lax.fori_loop(0, SLOTS // 2, step, 0)


def exchanged(value, axis):
    return lax.all_to_all(value, axis, split_axis=0, concat_axis=0, tiled=True)


def shifted(value, by):
    return lax.ppermute(value, "strip", [(i, (i + by) % PEERS) for i in range(PEERS)])


def body(
    image_in, cotangent, conv1_w, conv2_w, norm1_gain, norm1_shift, norm2_gain, norm2_shift, strip_rows
):
    x, g = image_in[0], cotangent[0]
    gain1, shift1 = norm1_gain[None], norm1_shift[None]
    gain2, shift2 = norm2_gain[None], norm2_shift[None]
    strip = lax.axis_index("strip")
    strip_id = strip.reshape(1).astype(jnp.int32)
    images = lax.axis_size(IMG)
    half = SLOTS // 2
    field = SLOTS * COLS * CH
    conv_flops = 2 * 9 * field * CH
    edge = (COLS, CH)
    stat = shape((PEERS, 8, CH), F32)

    top, bottom, stats1 = call(
        stats_kernel,
        [SMEM, HBM, HBM],
        [shape((2, *edge), BF16), shape((2, *edge), BF16), stat],
        flops=field * 6,
        moved=field * 2,
        scratch=[pltpu.VMEM((SLOTS, *edge), BF16), pltpu.SemaphoreType.DMA, pltpu.SemaphoreType.DMA((4,))],
        limit=63 * MIB + MIB // 4,
    )(strip_rows, x, g)
    up, down = shifted(bottom, 1), shifted(top, -1)
    weights1, turned1, turned2 = call(
        weights_kernel, [VMEM, VMEM], [shape((2, PAIR, 2 * CH), BF16)] * 3, flops=field * 2, moved=field
    )(conv1_w, conv2_w)
    stats1 = exchanged(stats1, "strip")

    hidden, act1, stats2 = call(
        hidden_kernel,
        [SMEM, SMEM] + [VMEM] * 7,
        [shape((SLOTS, *edge), F32), shape((half + 1, COLS, PAIR), BF16), stat],
        flops=conv_flops,
        moved=field * 6,
    )(strip_rows, strip_id, x, up, down, stats1, weights1, gain1, shift1)

    g_taps, back2, act1_t = call(
        back_kernel,
        [SMEM, SMEM] + [VMEM] * 5,
        [
            shape((half + 1, COLS, PAIR), BF16),
            shape((SLOTS, *edge), F32),
            shape((2, WIDE, (half + 2) * COLS), BF16),
        ],
        flops=conv_flops,
        moved=field * 6,
    )(strip_rows, strip_id, g, up, down, turned2, act1)
    stats2, g_taps, back2, act1_t = lax.optimization_barrier((stats2, g_taps, back2, act1_t))
    stats2 = exchanged(stats2, "strip")

    act2, dpre2, top, bottom, own_sums2 = call(
        dpre2_kernel,
        [SMEM] + [VMEM] * 5,
        [
            shape((SLOTS, *edge), BF16), shape((SLOTS, *edge), F32), shape((2, *edge), F32), shape((2, *edge), F32), stat,
        ],
        flops=field * 40,
        moved=field * 8,
    )(strip_rows, stats2, hidden, back2, gain2, shift2)
    up, down = shifted(bottom, 1), shifted(top, -1)

    (grad2,) = call(
        grad2_kernel,
        [SMEM] + [VMEM] * 2,
        [shape((WIDE, WIDE), F32)],
        flops=conv_flops,
        moved=field * 6,
        scratch=[pltpu.VMEM((2, WIDE, (half + 2) * COLS), BF16)],
    )(strip_rows, act2, g_taps)
    own_sums2, grad2 = lax.optimization_barrier((own_sums2, grad2))
    sums2 = exchanged(own_sums2, "strip")

    rows = 9 * CH // images
    share, dpre1, own_sums1 = call(
        dpre1_kernel,
        [SMEM, SMEM] + [VMEM] * 15,
        [shape((images, 2 * rows + 8, CH), BF16), shape((SLOTS, *edge), F32), shape((8, CH), F32)],
        flops=2 * conv_flops,
        moved=field * 8,
        scratch=[pltpu.VMEM((half + 1, COLS, PAIR), BF16), pltpu.VMEM((WIDE, WIDE), F32)],
    )(
        strip_rows, strip_id, stats1, stats2, sums2, own_sums2, hidden, dpre2, up, down, act1_t, x, grad2, turned1,
        gain1, shift1, gain2,
    )
    share, dpre1, own_sums1 = lax.optimization_barrier((share, dpre1, own_sums1))
    share = exchanged(share, IMG)
    (relayed,) = call(
        relay_kernel, [VMEM, VMEM], [shape((PEERS, 2 * rows + 16, CH), BF16)], moved=images * (2 * rows + 8) * CH * 2
    )(share, own_sums1)
    relayed = exchanged(relayed, "strip")
    image_grad, grad1, grad2, norm_grads = call(
        finish_kernel,
        [SMEM] + [VMEM] * 6,
        [shape((SLOTS, *edge), BF16), shape((rows, CH), F32), shape((rows, CH), F32), shape((4, CH), F32)],
        flops=field * 12,
        moved=field * 10,
    )(strip_rows, relayed, stats1, x, g, dpre1, gain1)
    return image_grad[None], grad1, grad2, norm_grads


def solution(mesh):
    torus = Mesh(mesh.devices.reshape(4, 4, 2, mesh.shape["strip"]), (*IMG, "strip"))
    return jax.shard_map(
        body,
        mesh=torus,
        in_specs=(
            P(IMG, "strip", None, None), P(IMG, "strip", None, None), P(), P(), P(), P(), P(), P(), P(IMG, "strip"),
        ),
        out_specs=(P(IMG, "strip", None, None), P(IMG, None), P(IMG, None), P()),
        check_vma=False,
    )
```

```python
import jax
import jax.numpy as jnp
from jax import lax
from jax.experimental import pallas as pl
from jax.experimental.pallas import tpu as pltpu
from jax.sharding import Mesh
from jax.sharding import PartitionSpec as P


IMG = ("img_0", "img_1", "img_2")
EPSILON = 1e-06
F32 = jnp.float32
BF16 = jnp.bfloat16
SLOTS = 32
COLS = 128
CH = 128
HEIGHT = 128
PER_GROUP = 4
PEERS = 8
CELLS = float(HEIGHT * COLS * PER_GROUP)
WIDE = 3 * CH
PAIR = 2 * WIDE
STEPS = 4
MIB = 1 << 20

VMEM = pl.BlockSpec(memory_space=pltpu.VMEM)
SMEM = pl.BlockSpec(memory_space=pltpu.SMEM)
HBM = pl.BlockSpec(memory_space=pltpu.HBM)


def shape(dims, dtype):
    return jax.ShapeDtypeStruct(dims, dtype)


def call(body, in_specs, outs, flops=0, moved=0, scratch=(), limit=12 * MIB, outs_in=None):
    return pl.pallas_call(
        body,
        in_specs=in_specs,
        out_specs=outs_in or [VMEM] * len(outs),
        out_shape=outs,
        scratch_shapes=scratch,
        compiler_params=pltpu.CompilerParams(vmem_limit_bytes=limit),
        cost_estimate=pl.CostEstimate(flops=flops, bytes_accessed=moved, transcendentals=0),
    )


def folded(row):
    lanes = jnp.broadcast_to(row, (8, CH))
    lane = lax.broadcasted_iota(jnp.int32, (8, CH), 1)
    lanes = lanes + jnp.where(lane % 2 == 0, pltpu.roll(lanes, CH - 1, 1), pltpu.roll(lanes, 1, 1))
    lanes = lanes + jnp.where(lane % 4 < 2, pltpu.roll(lanes, CH - 2, 1), pltpu.roll(lanes, 2, 1))
    return lanes[0:1]


def group_stats(stats):
    total = stats[0, 0:1]
    for j in range(1, PEERS):
        total = total + stats[j, 0:1]
    mean = folded(total) / CELLS
    spread = jnp.zeros((1, CH), F32)
    for j in range(PEERS):
        count = stats[j, 2:3] * float(COLS)
        gap = stats[j, 0:1] / count - mean
        spread = spread + stats[j, 1:2] + count * gap * gap
    return mean, lax.rsqrt(folded(spread) / CELLS + EPSILON)


def moments(sums, gain):
    cross, plain = sums[0, 0:1], sums[0, 1:2]
    for j in range(1, PEERS):
        cross, plain = cross + sums[j, 0:1], plain + sums[j, 1:2]
    return folded(cross * gain) / CELLS, folded(plain * gain) / CELLS


def sums8(value):
    return jnp.sum(value.reshape(-1, 8, value.shape[-1]), axis=0)


def send(out_ref, rows):
    index = lax.broadcasted_iota(jnp.int32, (8, CH), 0)
    tile = jnp.zeros((8, CH), F32)
    for k, row in enumerate(rows):
        tile = jnp.where(index == k, row, tile)
    for j in range(PEERS):
        out_ref[j] = tile


def kept_sums(value, r, length):
    return jnp.where(r < length, sums8(value), 0.0)


def channel_stats(load, length, out_ref, total=None):
    if total is None:
        total = sum(kept_sums(load(r), r, length) for r in range(SLOTS))
    total = jnp.sum(total, axis=0, keepdims=True)
    used = length.astype(F32)
    mean = total / (used * float(COLS))
    spread = jnp.zeros((8, CH), F32)
    for r in range(SLOTS):
        gap = load(r) - mean
        spread = spread + kept_sums(gap * gap, r, length)
    send(out_ref, [total, jnp.sum(spread, axis=0, keepdims=True), jnp.broadcast_to(used, (1, CH))])


def sigmoid(z):
    return 0.5 * jnp.tanh(0.5 * z) + 0.5


def taps(row):
    col = lax.broadcasted_iota(jnp.int32, (8, CH), 0)
    before, after = pltpu.roll(row, 1, 0), pltpu.roll(row, COLS - 1, 0)
    before = jnp.concatenate([jnp.where(col == 0, 0.0, before[0:8]), before[8:]], axis=0)
    after = jnp.concatenate([after[:-8], jnp.where(col == 7, 0.0, after[-8:])], axis=0)
    return jnp.concatenate([before.astype(BF16), row.astype(BF16), after.astype(BF16)], axis=1)


def convolve(buf, w_ref, row_at, finish, beside=lambda step: None, chunk=4):
    built = 0
    for begin in range(0, SLOTS // 2, chunk):
        needed = 2 * (begin + chunk) + 2
        for t in range(built, needed):
            buf[t // 2, :, t % 2 * WIDE : (t % 2 + 1) * WIDE] = taps(row_at(t))
        built = needed
        beside(begin // chunk)
        upper = buf[begin : begin + chunk].reshape(chunk * COLS, PAIR)
        lower = buf[begin + 1 : begin + 1 + chunk].reshape(chunk * COLS, PAIR)
        out = jnp.dot(
            jnp.concatenate([upper, lower], axis=1), w_ref[...].reshape(2 * PAIR, 2 * CH), preferred_element_type=F32
        )
        out = out.reshape(chunk, COLS, 2 * CH)
        for k in range(chunk):
            finish(2 * (begin + k), out[k, :, 0:CH])
            finish(2 * (begin + k) + 1, out[k, :, CH:])


def around(own, up, down, length, t):
    if t == 0:
        return up
    if t == SLOTS + 1:
        return down
    return jnp.where(t <= length, own(t - 1), down)


def in_image(length, strip, t):
    if t == 0:
        return strip > 0
    return (t <= length) | (strip < PEERS - 1)


def transposed_row(tile, i, ahead, keep, out_ref):
    tile = tile.T
    for tap in range(3):
        o = i + ahead - tap
        lanes = (o // 2 + 1) * COLS
        kept = jnp.where(keep(o), tile, jnp.zeros_like(tile))
        out_ref[o % 2, tap * CH : (tap + 1) * CH, lanes : lanes + COLS] = kept


def kernel_grad(rows_t, even, odd):
    used = slice(COLS, COLS + even.shape[0] * COLS)
    grad = jnp.dot(rows_t[0, :, used], even.reshape(-1, WIDE), preferred_element_type=F32)
    return grad + jnp.dot(rows_t[1, :, used], odd.reshape(-1, WIDE), preferred_element_type=F32)


def stats_kernel(len_ref, x_ref, g_ref, top_ref, bottom_ref, out_ref, rows_ref, sem, edge_sem):
    length = len_ref[0, 0]
    last = length - 1
    step = SLOTS // STEPS
    started = []
    for k in range(STEPS):
        part = pl.ds(k * step, step)
        started.append(pltpu.make_async_copy(x_ref.at[part], rows_ref.at[part], sem.at[k]))
    for k, ref in enumerate((x_ref, g_ref)):
        started.append(pltpu.make_async_copy(ref.at[0], top_ref.at[k], edge_sem.at[2 * k]))
        started.append(pltpu.make_async_copy(ref.at[last], bottom_ref.at[k], edge_sem.at[2 * k + 1]))
    for copy in started:
        copy.start()
    total = jnp.zeros((8, CH), F32)
    for k in range(STEPS):
        started[k].wait()
        for r in range(k * step, (k + 1) * step):
            total = total + kept_sums(rows_ref[r].astype(F32), r, length)
    channel_stats(lambda r: rows_ref[r].astype(F32), length, out_ref, total)
    for copy in started[STEPS:]:
        copy.wait()


def weights_kernel(first_ref, second_ref, ahead_ref, turned1_ref, turned2_ref):
    for out_ref in (ahead_ref, turned1_ref, turned2_ref):
        out_ref[0, WIDE * 0 : WIDE, CH : 2 * CH] = jnp.zeros((WIDE, CH), BF16)
        out_ref[1, WIDE:PAIR, 0:CH] = jnp.zeros((WIDE, CH), BF16)
    for a in range(3):
        for b in range(3):
            for v in range(2):
                half, lane = divmod((a + v) * WIDE + b * CH, PAIR)
                ahead_ref[half, lane : lane + CH, v * CH : (v + 1) * CH] = first_ref[a, b]
            for w_ref, out_ref in ((first_ref, turned1_ref), (second_ref, turned2_ref)):
                tile = w_ref[2 - a, 2 - b].T
                for v in range(2):
                    half, lane = divmod((a + v) * WIDE + b * CH, PAIR)
                    out_ref[half, lane : lane + CH, v * CH : (v + 1) * CH] = tile


def hidden_kernel(
    len_ref, x_ref, up_ref, down_ref, st_ref, w_ref, gain_ref, shift_ref, hid_ref, act_ref, out_ref
):
    length, strip = len_ref[0, 0], lax.axis_index("strip")
    mean, inv = group_stats(st_ref)
    scale, shift = inv * gain_ref[...], shift_ref[...]

    def row_at(t):
        row = around(lambda r: x_ref[r], up_ref[0], down_ref[0], length, t)
        pre = (row.astype(F32) - mean) * scale + shift
        return jnp.where(in_image(length, strip, t), pre * sigmoid(pre), 0.0)

    total = [jnp.zeros((8, CH), F32)]

    def finish(r, row):
        hid_ref[r] = row
        total[0] = total[0] + kept_sums(row, r, length)

    convolve(act_ref, w_ref, row_at, finish)
    channel_stats(lambda r: hid_ref[r], length, out_ref, total[0])


def back_kernel(len_ref, g_ref, up_ref, down_ref, w_ref, act_ref, g_taps_ref, back_ref, act_t_ref):
    length, strip = len_ref[0, 0], lax.axis_index("strip")

    def row_at(t):
        row = around(lambda r: g_ref[r], up_ref[1], down_ref[1], length, t)
        return jnp.where(in_image(length, strip, t), row.astype(F32), 0.0)

    def finish(r, row):
        back_ref[r] = row

    def beside(step):
        for i in range(step * 9, min(step * 9 + 9, SLOTS + 2)):
            tile = act_ref[i // 2, :, i % 2 * WIDE + CH : i % 2 * WIDE + 2 * CH]
            transposed_row(tile, i, 0, lambda o: (o >= 0) & (o < length), act_t_ref)

    convolve(g_taps_ref, w_ref, row_at, finish, beside)


def dpre2_kernel(
    len_ref, st_ref, hid_ref, back_ref, gain_ref, shift_ref, act_ref, dpre_ref, top_ref, bottom_ref, out_ref
):
    length = len_ref[0, 0]
    mean, inv = group_stats(st_ref)
    gain, shift = gain_ref[...], shift_ref[...]

    cross = plain = jnp.zeros((8, CH), F32)
    for r in range(SLOTS):
        normed = (hid_ref[r] - mean) * inv
        pre = normed * gain + shift
        s = sigmoid(pre)
        act = pre * s
        act_ref[r] = act.astype(BF16)
        grad = jnp.where(r < length, back_ref[r] * (s + act * (1.0 - s)), 0.0)
        dpre_ref[r] = grad
        plain = plain + sums8(grad)
        cross = cross + sums8(grad * normed)
    send(out_ref, [jnp.sum(cross, axis=0, keepdims=True), jnp.sum(plain, axis=0, keepdims=True)])
    for ref, row in ((top_ref, 0), (bottom_ref, length - 1)):
        ref[0] = dpre_ref[row]
        ref[1] = hid_ref[row]


def grad2_kernel(len_ref, act_ref, g_taps_ref, out_ref, act_t_ref):
    length = len_ref[0, 0]
    half = SLOTS // 2
    for tap, o in ((0, 0), (0, 1), (1, 0), (1, SLOTS + 1), (2, SLOTS), (2, SLOTS + 1)):
        lanes = (o // 2 + 1) * COLS
        act_t_ref[o % 2, tap * CH : (tap + 1) * CH, lanes : lanes + COLS] = jnp.zeros((CH, COLS), BF16)
    for i in range(SLOTS):
        transposed_row(act_ref[i], i, 2, lambda o: i < length, act_t_ref)
    out_ref[...] = kernel_grad(
        act_t_ref, g_taps_ref[0 : half + 1, :, 0:WIDE], g_taps_ref[0 : half + 1, :, WIDE:PAIR]
    )


def dpre1_kernel(
    len_ref, st1_ref, st2_ref, sums_ref, own_sums_ref, hid_ref, dpre2_ref, up_ref, down_ref, act_t_ref,
    x_ref, grad2_ref, w_ref, gain1_ref, shift1_ref, gain2_ref,
    share_ref, dpre_ref, out_ref, d_taps_ref, grad1_ref,
):
    length, strip = len_ref[0, 0], lax.axis_index("strip")
    half = SLOTS // 2
    mean2, inv2 = group_stats(st2_ref)
    gain2 = gain2_ref[...]
    cross2, plain2 = moments(sums_ref, gain2)

    by_dpre, by_hidden, level = inv2 * gain2, inv2 * inv2 * cross2, inv2 * plain2

    def dhidden(dpre, hidden):
        return dpre * by_dpre - (hidden - mean2) * by_hidden - level

    mean1, inv1 = group_stats(st1_ref)
    gain1, shift1 = gain1_ref[...], shift1_ref[...]
    sums = [jnp.zeros((8, CH), F32), jnp.zeros((8, CH), F32)]

    def row_at(t):
        dpre = around(lambda r: dpre2_ref[r], up_ref[0], down_ref[0], length, t)
        hidden = around(lambda r: hid_ref[r], up_ref[1], down_ref[1], length, t)
        return jnp.where(in_image(length, strip, t), dhidden(dpre, hidden), 0.0)

    def finish(r, row):
        normed = (x_ref[r].astype(F32) - mean1) * inv1
        pre = normed * gain1 + shift1
        s = sigmoid(pre)
        grad = jnp.where(r < length, row * (s + pre * s * (1.0 - s)), 0.0)
        dpre_ref[r] = grad
        sums[0] = sums[0] + sums8(grad * normed)
        sums[1] = sums[1] + sums8(grad)

    convolve(d_taps_ref, w_ref, row_at, finish)
    grad1_ref[...] = kernel_grad(act_t_ref, d_taps_ref[0:half, :, WIDE:PAIR], d_taps_ref[1 : half + 1, :, 0:WIDE])
    cross, plain = (jnp.sum(total, axis=0, keepdims=True) for total in sums)
    index = lax.broadcasted_iota(jnp.int32, (8, CH), 0)
    norm = jnp.where(index == 0, cross, jnp.where(index == 1, plain, 0.0))
    out_ref[...] = norm
    norm = norm + jnp.where(index == 2, own_sums_ref[0, 0:1], 0.0) + jnp.where(index == 3, own_sums_ref[0, 1:2], 0.0)
    blocks, rows = share_ref.shape[0], (share_ref.shape[1] - 8) // 2
    for j in range(blocks):
        share_ref[j] = packed(cut(grad1_ref, j * rows, rows), cut(grad2_ref, j * rows, rows), norm)


def cut(ref, begin, count):
    pieces = []
    while count:
        tap, row = divmod(begin, CH)
        here = min(count, CH - row)
        a, b = divmod(tap, 3)
        pieces.append(ref[a * CH + row : a * CH + row + here, (2 - b) * CH : (3 - b) * CH])
        begin, count = begin + here, count - here
    return pieces


def packed(first, second, norm):
    high = norm.astype(BF16).astype(F32)
    return jnp.concatenate([*first, *second, high[0:4], (norm - high)[0:4]], axis=0).astype(BF16)


def unpacked(total):
    rows = (total.shape[0] - 8) // 2
    norm = total[2 * rows : 2 * rows + 4] + total[2 * rows + 4 :]
    return total[0:rows], total[rows : 2 * rows], norm


def relay_kernel(in_ref, own_ref, out_ref):
    total = in_ref[0].astype(F32)
    for j in range(1, in_ref.shape[0]):
        total = total + in_ref[j].astype(F32)
    first, second, norm = unpacked(total)
    norm = jnp.concatenate([norm, jnp.zeros((4, CH), F32)], axis=0)
    own = own_ref[...]
    high = own.astype(BF16).astype(F32)
    image = jnp.concatenate([high[0:4], (own - high)[0:4]], axis=0).astype(BF16)
    tile = jnp.concatenate([packed([first], [second], norm), image], axis=0)
    for j in range(PEERS):
        out_ref[j] = tile


def finish_kernel(
    len_ref, in_ref, st_ref, x_ref, g_ref, dpre_ref, gain_ref, image_ref, first_ref, second_ref, norm_ref,
    rows_ref, first_own, second_own, norm_own, sem,
):
    total = in_ref[0].astype(F32)
    for j in range(1, PEERS):
        total = total + in_ref[j].astype(F32)
    rows = first_ref.shape[0]
    first_own[...], second_own[...], norm_own[...] = unpacked(total[0 : 2 * rows + 8])
    copies = []
    for k, (own, ref) in enumerate(((first_own, first_ref), (second_own, second_ref), (norm_own, norm_ref))):
        copies.append(pltpu.make_async_copy(own, ref, sem.at[STEPS + k]))
        copies[k].start()
    sums = total[2 * rows + 8 : 2 * rows + 12] + total[2 * rows + 12 : 2 * rows + 16]
    length = len_ref[0, 0]
    mean, inv = group_stats(st_ref)
    gain = gain_ref[...]
    cross, plain = folded(sums[0:1] * gain) / CELLS, folded(sums[1:2] * gain) / CELLS
    by_dpre, by_x, level = inv * gain, inv * inv * cross, inv * plain
    step = SLOTS // STEPS
    for k in range(STEPS):
        for r in range(k * step, (k + 1) * step):
            grad = dpre_ref[r] * by_dpre - (x_ref[r].astype(F32) - mean) * by_x - level
            rows_ref[r] = jnp.where(r < length, g_ref[r].astype(F32) + grad, 0.0).astype(BF16)
        part = pl.ds(k * step, step)
        copies.append(pltpu.make_async_copy(rows_ref.at[part], image_ref.at[part], sem.at[k]))
        copies[-1].start()
    for copy in copies:
        copy.wait()


def exchanged(value, axis):
    return lax.all_to_all(value, axis, split_axis=0, concat_axis=0, tiled=True)


def shifted(value, by):
    return lax.ppermute(value, "strip", [(i, (i + by) % PEERS) for i in range(PEERS)])


def body(
    image_in, cotangent, conv1_w, conv2_w, norm1_gain, norm1_shift, norm2_gain, norm2_shift, strip_rows
):
    x, g = image_in[0], cotangent[0]
    gain1, shift1 = norm1_gain[None], norm1_shift[None]
    gain2, shift2 = norm2_gain[None], norm2_shift[None]
    images = lax.axis_size(IMG)
    half = SLOTS // 2
    field = SLOTS * COLS * CH
    conv_flops = 2 * 9 * field * CH
    edge = (COLS, CH)
    stat = shape((PEERS, 8, CH), F32)

    top, bottom, stats1 = call(
        stats_kernel,
        [SMEM, HBM, HBM],
        [shape((2, *edge), BF16), shape((2, *edge), BF16), stat],
        flops=field * 6,
        moved=field * 2,
        scratch=[pltpu.VMEM((SLOTS, *edge), BF16), pltpu.SemaphoreType.DMA((STEPS,)), pltpu.SemaphoreType.DMA((4,))],
        limit=63 * MIB + MIB // 4,
    )(strip_rows, x, g)
    up, down = shifted(bottom, 1), shifted(top, -1)
    weights1, turned1, turned2 = call(
        weights_kernel, [VMEM, VMEM], [shape((2, PAIR, 2 * CH), BF16)] * 3, flops=field * 2, moved=field
    )(conv1_w, conv2_w)
    stats1 = exchanged(stats1, "strip")

    hidden, act1, stats2 = call(
        hidden_kernel,
        [SMEM] + [VMEM] * 7,
        [shape((SLOTS, *edge), F32), shape((half + 1, COLS, PAIR), BF16), stat],
        flops=conv_flops,
        moved=field * 6,
    )(strip_rows, x, up, down, stats1, weights1, gain1, shift1)

    g_taps, back2, act1_t = call(
        back_kernel,
        [SMEM] + [VMEM] * 5,
        [
            shape((half + 1, COLS, PAIR), BF16),
            shape((SLOTS, *edge), F32),
            shape((2, WIDE, (half + 2) * COLS), BF16),
        ],
        flops=conv_flops,
        moved=field * 6,
    )(strip_rows, g, up, down, turned2, act1)
    stats2, g_taps, back2, act1_t = lax.optimization_barrier((stats2, g_taps, back2, act1_t))
    stats2 = exchanged(stats2, "strip")

    act2, dpre2, top, bottom, own_sums2 = call(
        dpre2_kernel,
        [SMEM] + [VMEM] * 5,
        [
            shape((SLOTS, *edge), BF16), shape((SLOTS, *edge), F32), shape((2, *edge), F32), shape((2, *edge), F32), stat,
        ],
        flops=field * 40,
        moved=field * 8,
    )(strip_rows, stats2, hidden, back2, gain2, shift2)
    up, down = shifted(bottom, 1), shifted(top, -1)

    (grad2,) = call(
        grad2_kernel,
        [SMEM] + [VMEM] * 2,
        [shape((WIDE, WIDE), F32)],
        flops=conv_flops,
        moved=field * 6,
        scratch=[pltpu.VMEM((2, WIDE, (half + 2) * COLS), BF16)],
    )(strip_rows, act2, g_taps)
    own_sums2, grad2 = lax.optimization_barrier((own_sums2, grad2))
    sums2 = exchanged(own_sums2, "strip")

    rows = 9 * CH // images
    share, dpre1, own_sums1 = call(
        dpre1_kernel,
        [SMEM] + [VMEM] * 15,
        [shape((images, 2 * rows + 8, CH), BF16), shape((SLOTS, *edge), F32), shape((8, CH), F32)],
        flops=2 * conv_flops,
        moved=field * 8,
        scratch=[pltpu.VMEM((half + 1, COLS, PAIR), BF16), pltpu.VMEM((WIDE, WIDE), F32)],
    )(
        strip_rows, stats1, stats2, sums2, own_sums2, hidden, dpre2, up, down, act1_t, x, grad2, turned1,
        gain1, shift1, gain2,
    )
    share, dpre1, own_sums1 = lax.optimization_barrier((share, dpre1, own_sums1))
    share = exchanged(share, IMG)
    (relayed,) = call(
        relay_kernel, [VMEM, VMEM], [shape((PEERS, 2 * rows + 16, CH), BF16)], moved=images * (2 * rows + 8) * CH * 2
    )(share, own_sums1)
    relayed = exchanged(relayed, "strip")
    image_grad, grad1, grad2, norm_grads = call(
        finish_kernel,
        [SMEM] + [VMEM] * 6,
        [shape((SLOTS, *edge), BF16), shape((rows, CH), F32), shape((rows, CH), F32), shape((4, CH), F32)],
        flops=field * 12,
        moved=field * 10,
        scratch=[
            pltpu.VMEM((SLOTS, *edge), BF16), pltpu.VMEM((rows, CH), F32), pltpu.VMEM((rows, CH), F32),
            pltpu.VMEM((4, CH), F32), pltpu.SemaphoreType.DMA((STEPS + 3,)),
        ],
        outs_in=[HBM] * 4,
    )(strip_rows, relayed, stats1, x, g, dpre1, gain1)
    return image_grad[None], grad1, grad2, norm_grads


def solution(mesh):
    torus = Mesh(mesh.devices.reshape(4, 4, 2, mesh.shape["strip"]), (*IMG, "strip"))
    return jax.shard_map(
        body,
        mesh=torus,
        in_specs=(
            P(IMG, "strip", None, None), P(IMG, "strip", None, None), P(), P(), P(), P(), P(), P(), P(IMG, "strip"),
        ),
        out_specs=(P(IMG, "strip", None, None), P(IMG, None), P(IMG, None), P()),
        check_vma=False,
    )
```

```python
import jax
import jax.numpy as jnp
from jax import lax
from jax.experimental import pallas as pl
from jax.experimental.pallas import tpu as pltpu
from jax.sharding import Mesh
from jax.sharding import PartitionSpec as P


IMG = ("img_0", "img_1", "img_2")
EPSILON = 1e-06
F32 = jnp.float32
BF16 = jnp.bfloat16
SLOTS = 32
COLS = 128
CH = 128
HEIGHT = 128
PER_GROUP = 4
PEERS = 8
CELLS = float(HEIGHT * COLS * PER_GROUP)
WIDE = 3 * CH
PAIR = 2 * WIDE
STEPS = 4
MIB = 1 << 20

VMEM = pl.BlockSpec(memory_space=pltpu.VMEM)
SMEM = pl.BlockSpec(memory_space=pltpu.SMEM)
HBM = pl.BlockSpec(memory_space=pltpu.HBM)


def shape(dims, dtype):
    return jax.ShapeDtypeStruct(dims, dtype)


def call(body, in_specs, outs, flops=0, moved=0, scratch=(), limit=12 * MIB, outs_in=None, aliases=None):
    return pl.pallas_call(
        body,
        in_specs=in_specs,
        out_specs=outs_in or [VMEM] * len(outs),
        out_shape=outs,
        scratch_shapes=scratch,
        input_output_aliases=aliases or {},
        compiler_params=pltpu.CompilerParams(vmem_limit_bytes=limit),
        cost_estimate=pl.CostEstimate(flops=flops, bytes_accessed=moved, transcendentals=0),
    )


def folded(row):
    lanes = jnp.broadcast_to(row, (8, CH))
    lane = lax.broadcasted_iota(jnp.int32, (8, CH), 1)
    lanes = lanes + jnp.where(lane % 2 == 0, pltpu.roll(lanes, CH - 1, 1), pltpu.roll(lanes, 1, 1))
    lanes = lanes + jnp.where(lane % 4 < 2, pltpu.roll(lanes, CH - 2, 1), pltpu.roll(lanes, 2, 1))
    return lanes[0:1]


def group_stats(stats):
    total = stats[0, 0:1]
    for j in range(1, PEERS):
        total = total + stats[j, 0:1]
    mean = folded(total) / CELLS
    spread = jnp.zeros((1, CH), F32)
    for j in range(PEERS):
        count = stats[j, 2:3] * float(COLS)
        gap = stats[j, 0:1] / count - mean
        spread = spread + stats[j, 1:2] + count * gap * gap
    return mean, lax.rsqrt(folded(spread) / CELLS + EPSILON)


def moments(sums, gain):
    cross, plain = sums[0, 0:1], sums[0, 1:2]
    for j in range(1, PEERS):
        cross, plain = cross + sums[j, 0:1], plain + sums[j, 1:2]
    return folded(cross * gain) / CELLS, folded(plain * gain) / CELLS


def sums8(value):
    return jnp.sum(value.reshape(-1, 8, value.shape[-1]), axis=0)


def send(out_ref, rows):
    index = lax.broadcasted_iota(jnp.int32, (8, CH), 0)
    tile = jnp.zeros((8, CH), F32)
    for k, row in enumerate(rows):
        tile = jnp.where(index == k, row, tile)
    for j in range(PEERS):
        out_ref[j] = tile


def kept_sums(value, r, length):
    return jnp.where(r < length, sums8(value), 0.0)


def channel_stats(load, length, out_ref, total=None, more=()):
    if total is None:
        total = sum(kept_sums(load(r), r, length) for r in range(SLOTS))
    total = jnp.sum(total, axis=0, keepdims=True)
    used = length.astype(F32)
    mean = total / (used * float(COLS))
    spread = jnp.zeros((8, CH), F32)
    for r in range(SLOTS):
        gap = load(r) - mean
        spread = spread + kept_sums(gap * gap, r, length)
    send(out_ref, [total, jnp.sum(spread, axis=0, keepdims=True), jnp.broadcast_to(used, (1, CH)), *more])


def sigmoid(z):
    return 0.5 * jnp.tanh(0.5 * z) + 0.5


def taps(row):
    col = lax.broadcasted_iota(jnp.int32, (8, CH), 0)
    before, after = pltpu.roll(row, 1, 0), pltpu.roll(row, COLS - 1, 0)
    before = jnp.concatenate([jnp.where(col == 0, 0.0, before[0:8]), before[8:]], axis=0)
    after = jnp.concatenate([after[:-8], jnp.where(col == 7, 0.0, after[-8:])], axis=0)
    return jnp.concatenate([before.astype(BF16), row.astype(BF16), after.astype(BF16)], axis=1)


def convolve(buf, tile_of, pair_ref, row_at, finish, beside=lambda step: None, chunk=4):
    pair_ref[3 * WIDE :, 0:CH] = jnp.zeros((WIDE, CH), BF16)
    pair_ref[0:WIDE, CH:] = jnp.zeros((WIDE, CH), BF16)
    for tap in range(9):
        tile = tile_of(tap)
        pair_ref[tap * CH : (tap + 1) * CH, 0:CH] = tile
        pair_ref[WIDE + tap * CH : WIDE + (tap + 1) * CH, CH:] = tile
    built = 0
    for begin in range(0, SLOTS // 2, chunk):
        needed = 2 * (begin + chunk) + 2 if row_at else 0
        for t in range(built, needed):
            buf[t // 2, :, t % 2 * WIDE : (t % 2 + 1) * WIDE] = taps(row_at(t))
        built = needed
        beside(begin // chunk)
        upper = buf[begin : begin + chunk].reshape(chunk * COLS, PAIR)
        lower = buf[begin + 1 : begin + 1 + chunk].reshape(chunk * COLS, PAIR)
        out = jnp.dot(
            jnp.concatenate([upper, lower], axis=1), pair_ref[...], preferred_element_type=F32
        )
        out = out.reshape(chunk, COLS, 2 * CH)
        for k in range(chunk):
            finish(2 * (begin + k), out[k, :, 0:CH])
            finish(2 * (begin + k) + 1, out[k, :, CH:])


def ahead(w_ref):
    return lambda tap: w_ref[tap * CH : (tap + 1) * CH]


def turned(w_ref):
    return lambda tap: w_ref[(8 - tap) * CH : (9 - tap) * CH].T


def place_halo(buf, length, above, below):
    buf[0, :, 0:WIDE] = above
    pair = (length + 1) // 2

    @pl.when(length % 2 == 1)
    def _():
        buf[pair, :, 0:WIDE] = below

    @pl.when(length % 2 == 0)
    def _():
        buf[pair, :, WIDE:PAIR] = below


def around(own, up, down, length, t):
    if t == 0:
        return up
    if t == SLOTS + 1:
        return down
    return jnp.where(t <= length, own(t - 1), down)


def in_image(length, strip, t):
    if t == 0:
        return strip > 0
    return (t <= length) | (strip < PEERS - 1)


def transposed_row(tile, i, ahead, keep, out_ref):
    tile = tile.T
    for tap in range(3):
        o = i + ahead - tap
        lanes = (o // 2 + 1) * COLS
        kept = jnp.where(keep(o), tile, jnp.zeros_like(tile))
        out_ref[o % 2, tap * CH : (tap + 1) * CH, lanes : lanes + COLS] = kept


def kernel_grad(rows_t, even, odd):
    used = slice(COLS, COLS + even.shape[0] * COLS)
    grad = jnp.dot(rows_t[0, :, used], even.reshape(-1, WIDE), preferred_element_type=F32)
    return grad + jnp.dot(rows_t[1, :, used], odd.reshape(-1, WIDE), preferred_element_type=F32)


def stats_kernel(
    len_ref, x_ref, g_ref, gain_ref, shift_ref, top_ref, bottom_ref, out_ref,
    rows_ref, gain_own, shift_own, sem, edge_sem, param_sem,
):
    length = len_ref[0, 0]
    last = length - 1
    step = SLOTS // STEPS
    started = []
    for k in range(STEPS):
        part = pl.ds(k * step, step)
        started.append(pltpu.make_async_copy(x_ref.at[part], rows_ref.at[part], sem.at[k]))
    for k, ref in enumerate((x_ref, g_ref)):
        started.append(pltpu.make_async_copy(ref.at[0], top_ref.at[k], edge_sem.at[2 * k]))
        started.append(pltpu.make_async_copy(ref.at[last], bottom_ref.at[k], edge_sem.at[2 * k + 1]))
    for copy in started:
        copy.start()
    params = ((gain_ref, gain_own), (shift_ref, shift_own))
    params = [pltpu.make_async_copy(ref, own, param_sem.at[k]) for k, (ref, own) in enumerate(params)]
    for copy in params:
        copy.start()
    total = jnp.zeros((8, CH), F32)
    for k in range(STEPS):
        started[k].wait()
        for r in range(k * step, (k + 1) * step):
            total = total + kept_sums(rows_ref[r].astype(F32), r, length)
    for copy in params:
        copy.wait()
    more = [gain_own[...], shift_own[...]]
    channel_stats(lambda r: rows_ref[r].astype(F32), length, out_ref, total, more)
    for copy in started[STEPS:]:
        copy.wait()


def act1_of(st_ref):
    mean, inv = group_stats(st_ref)
    scale, shift = inv * st_ref[0, 3:4], st_ref[0, 4:5]

    def act(row):
        pre = (row.astype(F32) - mean) * scale + shift
        return pre * sigmoid(pre)

    return act


def act1_kernel(x_ref, st_ref, act_ref):
    act = act1_of(st_ref)
    act_ref[0, :, 0:WIDE] = jnp.zeros((COLS, WIDE), BF16)
    act_ref[SLOTS // 2, :, WIDE:PAIR] = jnp.zeros((COLS, WIDE), BF16)
    for t in range(1, SLOTS + 1):
        act_ref[t // 2, :, t % 2 * WIDE : (t % 2 + 1) * WIDE] = taps(act(x_ref[t - 1]))


def hidden_kernel(
    len_ref, own_ref, up_ref, down_ref, st_ref, w_ref, hid_ref, act_ref, out_ref, pair_ref
):
    del own_ref
    length, strip = len_ref[0, 0], lax.axis_index("strip")
    act = act1_of(st_ref)
    place_halo(
        act_ref,
        length,
        taps(jnp.where(strip > 0, act(up_ref[0]), 0.0)),
        taps(jnp.where(strip < PEERS - 1, act(down_ref[0]), 0.0)),
    )
    total = [jnp.zeros((8, CH), F32)]

    def finish(r, row):
        hid_ref[r] = row
        total[0] = total[0] + kept_sums(row, r, length)

    convolve(act_ref, ahead(w_ref), pair_ref, None, finish)
    channel_stats(lambda r: hid_ref[r], length, out_ref, total[0])


def back_kernel(len_ref, g_ref, up_ref, down_ref, w_ref, act_ref, g_taps_ref, back_ref, act_t_ref, pair_ref):
    length, strip = len_ref[0, 0], lax.axis_index("strip")

    def row_at(t):
        row = around(lambda r: g_ref[r], up_ref[1], down_ref[1], length, t)
        return jnp.where(in_image(length, strip, t), row.astype(F32), 0.0)

    def finish(r, row):
        back_ref[r] = row

    def beside(step):
        for i in range(step * 9, min(step * 9 + 9, SLOTS + 2)):
            tile = act_ref[i // 2, :, i % 2 * WIDE + CH : i % 2 * WIDE + 2 * CH]
            transposed_row(tile, i, 0, lambda o: (o >= 0) & (o < length), act_t_ref)

    convolve(g_taps_ref, turned(w_ref), pair_ref, row_at, finish, beside)


def dpre2_kernel(
    len_ref, st_ref, hid_ref, back_ref, gain_ref, shift_ref, act_ref, dpre_ref, top_ref, bottom_ref, out_ref
):
    length = len_ref[0, 0]
    mean, inv = group_stats(st_ref)
    gain, shift = gain_ref[...], shift_ref[...]

    cross = plain = jnp.zeros((8, CH), F32)
    for r in range(SLOTS):
        normed = (hid_ref[r] - mean) * inv
        pre = normed * gain + shift
        s = sigmoid(pre)
        act = pre * s
        act_ref[r] = act.astype(BF16)
        grad = jnp.where(r < length, back_ref[r] * (s + act * (1.0 - s)), 0.0)
        dpre_ref[r] = grad
        plain = plain + sums8(grad)
        cross = cross + sums8(grad * normed)
    send(out_ref, [jnp.sum(cross, axis=0, keepdims=True), jnp.sum(plain, axis=0, keepdims=True)])
    for ref, row in ((top_ref, 0), (bottom_ref, length - 1)):
        ref[0] = dpre_ref[row]
        ref[1] = hid_ref[row]


def grad2_kernel(len_ref, act_ref, g_taps_ref, out_ref, act_t_ref):
    length = len_ref[0, 0]
    half = SLOTS // 2
    for tap, o in ((0, 0), (0, 1), (1, 0), (1, SLOTS + 1), (2, SLOTS), (2, SLOTS + 1)):
        lanes = (o // 2 + 1) * COLS
        act_t_ref[o % 2, tap * CH : (tap + 1) * CH, lanes : lanes + COLS] = jnp.zeros((CH, COLS), BF16)
    for i in range(SLOTS):
        transposed_row(act_ref[i], i, 2, lambda o: i < length, act_t_ref)
    out_ref[...] = kernel_grad(
        act_t_ref, g_taps_ref[0 : half + 1, :, 0:WIDE], g_taps_ref[0 : half + 1, :, WIDE:PAIR]
    )


def dpre1_kernel(
    len_ref, st1_ref, st2_ref, sums_ref, own_sums_ref, hid_ref, dpre2_ref, up_ref, down_ref, act_t_ref,
    x_ref, grad2_ref, w_ref, gain1_ref, shift1_ref, gain2_ref,
    share_ref, dpre_ref, out_ref, d_taps_ref, grad1_ref, pair_ref,
):
    length, strip = len_ref[0, 0], lax.axis_index("strip")
    half = SLOTS // 2
    mean2, inv2 = group_stats(st2_ref)
    gain2 = gain2_ref[...]
    cross2, plain2 = moments(sums_ref, gain2)

    by_dpre, by_hidden, level = inv2 * gain2, inv2 * inv2 * cross2, inv2 * plain2

    def dhidden(dpre, hidden):
        return dpre * by_dpre - (hidden - mean2) * by_hidden - level

    mean1, inv1 = group_stats(st1_ref)
    gain1, shift1 = gain1_ref[...], shift1_ref[...]
    sums = [jnp.zeros((8, CH), F32), jnp.zeros((8, CH), F32)]

    def row_at(t):
        dpre = around(lambda r: dpre2_ref[r], up_ref[0], down_ref[0], length, t)
        hidden = around(lambda r: hid_ref[r], up_ref[1], down_ref[1], length, t)
        return jnp.where(in_image(length, strip, t), dhidden(dpre, hidden), 0.0)

    def finish(r, row):
        normed = (x_ref[r].astype(F32) - mean1) * inv1
        pre = normed * gain1 + shift1
        s = sigmoid(pre)
        grad = jnp.where(r < length, row * (s + pre * s * (1.0 - s)), 0.0)
        dpre_ref[r] = grad
        sums[0] = sums[0] + sums8(grad * normed)
        sums[1] = sums[1] + sums8(grad)

    convolve(d_taps_ref, turned(w_ref), pair_ref, row_at, finish, chunk=1)
    grad1_ref[...] = kernel_grad(act_t_ref, d_taps_ref[0:half, :, WIDE:PAIR], d_taps_ref[1 : half + 1, :, 0:WIDE])
    cross, plain = (jnp.sum(total, axis=0, keepdims=True) for total in sums)
    index = lax.broadcasted_iota(jnp.int32, (8, CH), 0)
    norm = jnp.where(index == 0, cross, jnp.where(index == 1, plain, 0.0))
    out_ref[...] = norm
    norm = norm + jnp.where(index == 2, own_sums_ref[0, 0:1], 0.0) + jnp.where(index == 3, own_sums_ref[0, 1:2], 0.0)
    blocks, rows = share_ref.shape[0], (share_ref.shape[1] - 8) // 2
    for j in range(blocks):
        share_ref[j] = packed(cut(grad1_ref, j * rows, rows), cut(grad2_ref, j * rows, rows), norm)


def cut(ref, begin, count):
    pieces = []
    while count:
        tap, row = divmod(begin, CH)
        here = min(count, CH - row)
        a, b = divmod(tap, 3)
        pieces.append(ref[a * CH + row : a * CH + row + here, (2 - b) * CH : (3 - b) * CH])
        begin, count = begin + here, count - here
    return pieces


def packed(first, second, norm):
    high = norm.astype(BF16).astype(F32)
    return jnp.concatenate([*first, *second, high[0:4], (norm - high)[0:4]], axis=0).astype(BF16)


def unpacked(total):
    rows = (total.shape[0] - 8) // 2
    norm = total[2 * rows : 2 * rows + 4] + total[2 * rows + 4 :]
    return total[0:rows], total[rows : 2 * rows], norm


def relay_kernel(in_ref, own_ref, out_ref):
    total = in_ref[0].astype(F32)
    for j in range(1, in_ref.shape[0]):
        total = total + in_ref[j].astype(F32)
    first, second, norm = unpacked(total)
    norm = jnp.concatenate([norm, jnp.zeros((4, CH), F32)], axis=0)
    own = own_ref[...]
    high = own.astype(BF16).astype(F32)
    image = jnp.concatenate([high[0:4], (own - high)[0:4]], axis=0).astype(BF16)
    tile = jnp.concatenate([packed([first], [second], norm), image], axis=0)
    for j in range(PEERS):
        out_ref[j] = tile


def finish_kernel(
    len_ref, in_ref, st_ref, x_ref, g_ref, dpre_ref, gain_ref, image_ref, first_ref, second_ref, norm_ref,
    rows_ref, first_own, second_own, norm_own, sem,
):
    total = in_ref[0].astype(F32)
    for j in range(1, PEERS):
        total = total + in_ref[j].astype(F32)
    rows = first_ref.shape[0]
    first_own[...], second_own[...], norm_own[...] = unpacked(total[0 : 2 * rows + 8])
    copies = []
    for k, (own, ref) in enumerate(((first_own, first_ref), (second_own, second_ref), (norm_own, norm_ref))):
        copies.append(pltpu.make_async_copy(own, ref, sem.at[STEPS + k]))
        copies[k].start()
    sums = total[2 * rows + 8 : 2 * rows + 12] + total[2 * rows + 12 : 2 * rows + 16]
    length = len_ref[0, 0]
    mean, inv = group_stats(st_ref)
    gain = gain_ref[...]
    cross, plain = folded(sums[0:1] * gain) / CELLS, folded(sums[1:2] * gain) / CELLS
    by_dpre, by_x, level = inv * gain, inv * inv * cross, inv * plain
    step = SLOTS // STEPS
    for k in range(STEPS):
        for r in range(k * step, (k + 1) * step):
            grad = dpre_ref[r] * by_dpre - (x_ref[r].astype(F32) - mean) * by_x - level
            rows_ref[r] = jnp.where(r < length, g_ref[r].astype(F32) + grad, 0.0).astype(BF16)
        part = pl.ds(k * step, step)
        copies.append(pltpu.make_async_copy(rows_ref.at[part], image_ref.at[part], sem.at[k]))
        copies[-1].start()
    for copy in copies:
        copy.wait()


def exchanged(value, axis):
    return lax.all_to_all(value, axis, split_axis=0, concat_axis=0, tiled=True)


def shifted(value, by):
    return lax.ppermute(value, "strip", [(i, (i + by) % PEERS) for i in range(PEERS)])


def body(
    image_in, cotangent, conv1_w, conv2_w, norm1_gain, norm1_shift, norm2_gain, norm2_shift, strip_rows
):
    x, g = image_in[0], cotangent[0]
    gain1, shift1 = norm1_gain[None], norm1_shift[None]
    gain2, shift2 = norm2_gain[None], norm2_shift[None]
    images = lax.axis_size(IMG)
    half = SLOTS // 2
    field = SLOTS * COLS * CH
    conv_flops = 2 * 9 * field * CH
    edge = (COLS, CH)
    stat = shape((PEERS, 8, CH), F32)

    ahead1, ahead2 = conv1_w.reshape(9 * CH, CH), conv2_w.reshape(9 * CH, CH)
    pair = pltpu.VMEM((2 * PAIR, 2 * CH), BF16)
    top, bottom, stats1 = call(
        stats_kernel,
        [SMEM] + [HBM] * 4,
        [shape((2, *edge), BF16), shape((2, *edge), BF16), stat],
        flops=field * 6,
        moved=field * 2,
        scratch=[
            pltpu.VMEM((SLOTS, *edge), BF16), pltpu.VMEM((1, CH), F32), pltpu.VMEM((1, CH), F32),
            pltpu.SemaphoreType.DMA((STEPS,)), pltpu.SemaphoreType.DMA((4,)), pltpu.SemaphoreType.DMA((2,)),
        ],
        limit=63 * MIB + MIB // 4,
    )(strip_rows, x, g, gain1, shift1)
    up, down = shifted(bottom, 1), shifted(top, -1)
    stats1 = exchanged(stats1, "strip")

    (act1,) = call(
        act1_kernel, [VMEM] * 2, [shape((half + 1, COLS, PAIR), BF16)], flops=field * 20, moved=field * 4
    )(x, stats1)
    hidden, act1, stats2 = call(
        hidden_kernel,
        [SMEM] + [VMEM] * 5,
        [shape((SLOTS, *edge), F32), shape((half + 1, COLS, PAIR), BF16), stat],
        flops=conv_flops,
        moved=field * 6,
        scratch=[pair],
        aliases={1: 1},
    )(strip_rows, act1, up, down, stats1, ahead1)

    g_taps, back2, act1_t = call(
        back_kernel,
        [SMEM] + [VMEM] * 5,
        [
            shape((half + 1, COLS, PAIR), BF16),
            shape((SLOTS, *edge), F32),
            shape((2, WIDE, (half + 2) * COLS), BF16),
        ],
        flops=conv_flops,
        moved=field * 6,
        scratch=[pair],
    )(strip_rows, g, up, down, ahead2, act1)
    stats2, g_taps, back2, act1_t = lax.optimization_barrier((stats2, g_taps, back2, act1_t))
    stats2 = exchanged(stats2, "strip")

    act2, dpre2, top, bottom, own_sums2 = call(
        dpre2_kernel,
        [SMEM] + [VMEM] * 5,
        [
            shape((SLOTS, *edge), BF16), shape((SLOTS, *edge), F32), shape((2, *edge), F32), shape((2, *edge), F32), stat,
        ],
        flops=field * 40,
        moved=field * 8,
    )(strip_rows, stats2, hidden, back2, gain2, shift2)
    up, down = shifted(bottom, 1), shifted(top, -1)

    (grad2,) = call(
        grad2_kernel,
        [SMEM] + [VMEM] * 2,
        [shape((WIDE, WIDE), F32)],
        flops=conv_flops,
        moved=field * 6,
        scratch=[pltpu.VMEM((2, WIDE, (half + 2) * COLS), BF16)],
    )(strip_rows, act2, g_taps)
    own_sums2, grad2 = lax.optimization_barrier((own_sums2, grad2))
    sums2 = exchanged(own_sums2, "strip")

    rows = 9 * CH // images
    share, dpre1, own_sums1 = call(
        dpre1_kernel,
        [SMEM] + [VMEM] * 15,
        [shape((images, 2 * rows + 8, CH), BF16), shape((SLOTS, *edge), F32), shape((8, CH), F32)],
        flops=2 * conv_flops,
        moved=field * 8,
        scratch=[pltpu.VMEM((half + 1, COLS, PAIR), BF16), pltpu.VMEM((WIDE, WIDE), F32), pair],
    )(
        strip_rows, stats1, stats2, sums2, own_sums2, hidden, dpre2, up, down, act1_t, x, grad2, ahead1,
        gain1, shift1, gain2,
    )
    share, dpre1, own_sums1 = lax.optimization_barrier((share, dpre1, own_sums1))
    share = exchanged(share, IMG)
    (relayed,) = call(
        relay_kernel, [VMEM, VMEM], [shape((PEERS, 2 * rows + 16, CH), BF16)], moved=images * (2 * rows + 8) * CH * 2
    )(share, own_sums1)
    relayed = exchanged(relayed, "strip")
    image_grad, grad1, grad2, norm_grads = call(
        finish_kernel,
        [SMEM] + [VMEM] * 6,
        [shape((SLOTS, *edge), BF16), shape((rows, CH), F32), shape((rows, CH), F32), shape((4, CH), F32)],
        flops=field * 12,
        moved=field * 10,
        scratch=[
            pltpu.VMEM((SLOTS, *edge), BF16), pltpu.VMEM((rows, CH), F32), pltpu.VMEM((rows, CH), F32),
            pltpu.VMEM((4, CH), F32), pltpu.SemaphoreType.DMA((STEPS + 3,)),
        ],
        outs_in=[HBM] * 4,
    )(strip_rows, relayed, stats1, x, g, dpre1, gain1)
    return image_grad[None], grad1, grad2, norm_grads


def solution(mesh):
    torus = Mesh(mesh.devices.reshape(4, 4, 2, mesh.shape["strip"]), (*IMG, "strip"))
    return jax.shard_map(
        body,
        mesh=torus,
        in_specs=(
            P(IMG, "strip", None, None), P(IMG, "strip", None, None), P(), P(), P(), P(), P(), P(), P(IMG, "strip"),
        ),
        out_specs=(P(IMG, "strip", None, None), P(IMG, None), P(IMG, None), P()),
        check_vma=False,
    )
```

```python
import jax
import jax.numpy as jnp
from jax import lax
from jax.experimental import pallas as pl
from jax.experimental.pallas import tpu as pltpu
from jax.sharding import Mesh
from jax.sharding import PartitionSpec as P


IMG = ("img_0", "img_1", "img_2")
EPSILON = 1e-06
F32 = jnp.float32
BF16 = jnp.bfloat16
SLOTS = 32
COLS = 128
CH = 128
HEIGHT = 128
PER_GROUP = 4
PEERS = 8
CELLS = float(HEIGHT * COLS * PER_GROUP)
WIDE = 3 * CH
PAIR = 2 * WIDE
STEPS = 4
MIB = 1 << 20

VMEM = pl.BlockSpec(memory_space=pltpu.VMEM)
SMEM = pl.BlockSpec(memory_space=pltpu.SMEM)
HBM = pl.BlockSpec(memory_space=pltpu.HBM)


def shape(dims, dtype):
    return jax.ShapeDtypeStruct(dims, dtype)


def call(body, in_specs, outs, flops=0, moved=0, scratch=(), limit=12 * MIB, outs_in=None, aliases=None):
    return pl.pallas_call(
        body,
        in_specs=in_specs,
        out_specs=outs_in or [VMEM] * len(outs),
        out_shape=outs,
        scratch_shapes=scratch,
        input_output_aliases=aliases or {},
        compiler_params=pltpu.CompilerParams(vmem_limit_bytes=limit),
        cost_estimate=pl.CostEstimate(flops=flops, bytes_accessed=moved, transcendentals=0),
    )


def folded(row):
    lanes = jnp.broadcast_to(row, (8, CH))
    lane = lax.broadcasted_iota(jnp.int32, (8, CH), 1)
    lanes = lanes + jnp.where(lane % 2 == 0, pltpu.roll(lanes, CH - 1, 1), pltpu.roll(lanes, 1, 1))
    lanes = lanes + jnp.where(lane % 4 < 2, pltpu.roll(lanes, CH - 2, 1), pltpu.roll(lanes, 2, 1))
    return lanes[0:1]


def group_stats(stats):
    total = stats[0, 0:1]
    for j in range(1, PEERS):
        total = total + stats[j, 0:1]
    mean = folded(total) / CELLS
    spread = jnp.zeros((1, CH), F32)
    for j in range(PEERS):
        count = stats[j, 2:3] * float(COLS)
        gap = stats[j, 0:1] / count - mean
        spread = spread + stats[j, 1:2] + count * gap * gap
    return mean, lax.rsqrt(folded(spread) / CELLS + EPSILON)


def moments(sums, gain):
    cross, plain = sums[0, 0:1], sums[0, 1:2]
    for j in range(1, PEERS):
        cross, plain = cross + sums[j, 0:1], plain + sums[j, 1:2]
    return folded(cross * gain) / CELLS, folded(plain * gain) / CELLS


def sums8(value):
    return jnp.sum(value.reshape(-1, 8, value.shape[-1]), axis=0)


def send(out_ref, rows):
    index = lax.broadcasted_iota(jnp.int32, (8, CH), 0)
    tile = jnp.zeros((8, CH), F32)
    for k, row in enumerate(rows):
        tile = jnp.where(index == k, row, tile)
    for j in range(PEERS):
        out_ref[j] = tile


def kept_sums(value, r, length):
    return jnp.where(r < length, sums8(value), 0.0)


def channel_stats(load, length, out_ref, total=None, more=()):
    if total is None:
        total = sum(kept_sums(load(r), r, length) for r in range(SLOTS))
    total = jnp.sum(total, axis=0, keepdims=True)
    used = length.astype(F32)
    mean = total / (used * float(COLS))
    spread = jnp.zeros((8, CH), F32)
    for r in range(SLOTS):
        gap = load(r) - mean
        spread = spread + kept_sums(gap * gap, r, length)
    send(out_ref, [total, jnp.sum(spread, axis=0, keepdims=True), jnp.broadcast_to(used, (1, CH)), *more])


def silu_parts(half):
    t = jnp.tanh(half)
    act = half * (1.0 + t)
    return act, 0.5 * ((1.0 + t) + act * (1.0 - t))


def taps(row):
    col = lax.broadcasted_iota(jnp.int32, (8, CH), 0)
    before, after = pltpu.roll(row, 1, 0), pltpu.roll(row, COLS - 1, 0)
    before = jnp.concatenate([jnp.where(col == 0, 0.0, before[0:8]), before[8:]], axis=0)
    after = jnp.concatenate([after[:-8], jnp.where(col == 7, 0.0, after[-8:])], axis=0)
    return jnp.concatenate([before.astype(BF16), row.astype(BF16), after.astype(BF16)], axis=1)


def convolve(buf, tile_of, pair_ref, row_at, finish, beside=lambda step: None, chunk=4):
    pair_ref[3 * WIDE :, 0:CH] = jnp.zeros((WIDE, CH), BF16)
    pair_ref[0:WIDE, CH:] = jnp.zeros((WIDE, CH), BF16)
    for tap in range(9):
        tile = tile_of(tap)
        pair_ref[tap * CH : (tap + 1) * CH, 0:CH] = tile
        pair_ref[WIDE + tap * CH : WIDE + (tap + 1) * CH, CH:] = tile
    built = 0
    for begin in range(0, SLOTS // 2, chunk):
        needed = 2 * (begin + chunk) + 2 if row_at else 0
        for t in range(built, needed):
            buf[t // 2, :, t % 2 * WIDE : (t % 2 + 1) * WIDE] = taps(row_at(t))
        built = needed
        beside(begin // chunk)
        upper = buf[begin : begin + chunk].reshape(chunk * COLS, PAIR)
        lower = buf[begin + 1 : begin + 1 + chunk].reshape(chunk * COLS, PAIR)
        out = jnp.dot(
            jnp.concatenate([upper, lower], axis=1), pair_ref[...], preferred_element_type=F32
        )
        out = out.reshape(chunk, COLS, 2 * CH)
        for k in range(chunk):
            finish(2 * (begin + k), out[k, :, 0:CH])
            finish(2 * (begin + k) + 1, out[k, :, CH:])


def ahead(w_ref):
    return lambda tap: w_ref[tap * CH : (tap + 1) * CH]


def turned(w_ref):
    return lambda tap: w_ref[(8 - tap) * CH : (9 - tap) * CH].T


def place_halo(buf, length, above, below):
    buf[0, :, 0:WIDE] = above
    pair = (length + 1) // 2

    @pl.when(length % 2 == 1)
    def _():
        buf[pair, :, 0:WIDE] = below

    @pl.when(length % 2 == 0)
    def _():
        buf[pair, :, WIDE:PAIR] = below


def around(own, up, down, length, t):
    if t == 0:
        return up
    if t == SLOTS + 1:
        return down
    return jnp.where(t <= length, own(t - 1), down)


def in_image(length, strip, t):
    if t == 0:
        return strip > 0
    return (t <= length) | (strip < PEERS - 1)


def transposed_row(tile, i, ahead, keep, out_ref):
    tile = tile.T
    for tap in range(3):
        o = i + ahead - tap
        lanes = (o // 2 + 1) * COLS
        kept = jnp.where(keep(o), tile, jnp.zeros_like(tile))
        out_ref[o % 2, tap * CH : (tap + 1) * CH, lanes : lanes + COLS] = kept


def kernel_grad(rows_t, even, odd):
    used = slice(COLS, COLS + even.shape[0] * COLS)
    grad = jnp.dot(rows_t[0, :, used], even.reshape(-1, WIDE), preferred_element_type=F32)
    return grad + jnp.dot(rows_t[1, :, used], odd.reshape(-1, WIDE), preferred_element_type=F32)


def stats_kernel(
    len_ref, x_ref, g_ref, gain_ref, shift_ref, top_ref, bottom_ref, out_ref,
    rows_ref, gain_own, shift_own, sem, edge_sem, param_sem,
):
    length = len_ref[0, 0]
    last = length - 1
    step = SLOTS // STEPS
    started = []
    for k in range(STEPS):
        part = pl.ds(k * step, step)
        started.append(pltpu.make_async_copy(x_ref.at[part], rows_ref.at[part], sem.at[k]))
    for k, ref in enumerate((x_ref, g_ref)):
        started.append(pltpu.make_async_copy(ref.at[0], top_ref.at[k], edge_sem.at[2 * k]))
        started.append(pltpu.make_async_copy(ref.at[last], bottom_ref.at[k], edge_sem.at[2 * k + 1]))
    for copy in started:
        copy.start()
    params = ((gain_ref, gain_own), (shift_ref, shift_own))
    params = [pltpu.make_async_copy(ref, own, param_sem.at[k]) for k, (ref, own) in enumerate(params)]
    for copy in params:
        copy.start()
    total = jnp.zeros((8, CH), F32)
    for k in range(STEPS):
        started[k].wait()
        for r in range(k * step, (k + 1) * step):
            total = total + kept_sums(rows_ref[r].astype(F32), r, length)
    for copy in params:
        copy.wait()
    more = [gain_own[...], shift_own[...]]
    channel_stats(lambda r: rows_ref[r].astype(F32), length, out_ref, total, more)
    for copy in started[STEPS:]:
        copy.wait()


def act1_of(st_ref):
    mean, inv = group_stats(st_ref)
    scale, shift = 0.5 * (inv * st_ref[0, 3:4]), 0.5 * st_ref[0, 4:5]

    def act(row):
        return silu_parts((row.astype(F32) - mean) * scale + shift)[0]

    return act


def act1_kernel(x_ref, st_ref, act_ref):
    act = act1_of(st_ref)
    act_ref[0, :, 0:WIDE] = jnp.zeros((COLS, WIDE), BF16)
    act_ref[SLOTS // 2, :, WIDE:PAIR] = jnp.zeros((COLS, WIDE), BF16)
    for t in range(1, SLOTS + 1):
        act_ref[t // 2, :, t % 2 * WIDE : (t % 2 + 1) * WIDE] = taps(act(x_ref[t - 1]))


def hidden_kernel(
    len_ref, own_ref, up_ref, down_ref, st_ref, w_ref, hid_ref, act_ref, out_ref, pair_ref
):
    del own_ref
    length, strip = len_ref[0, 0], lax.axis_index("strip")
    act = act1_of(st_ref)
    place_halo(
        act_ref,
        length,
        taps(jnp.where(strip > 0, act(up_ref[0]), 0.0)),
        taps(jnp.where(strip < PEERS - 1, act(down_ref[0]), 0.0)),
    )
    total = [jnp.zeros((8, CH), F32)]

    def finish(r, row):
        hid_ref[r] = row
        total[0] = total[0] + kept_sums(row, r, length)

    convolve(act_ref, ahead(w_ref), pair_ref, None, finish)
    channel_stats(lambda r: hid_ref[r], length, out_ref, total[0])


def back_kernel(len_ref, g_ref, up_ref, down_ref, w_ref, act_ref, g_taps_ref, back_ref, act_t_ref, pair_ref):
    length, strip = len_ref[0, 0], lax.axis_index("strip")

    def row_at(t):
        row = around(lambda r: g_ref[r], up_ref[1], down_ref[1], length, t)
        return jnp.where(in_image(length, strip, t), row.astype(F32), 0.0)

    def finish(r, row):
        back_ref[r] = row

    def beside(step):
        for i in range(step * 9, min(step * 9 + 9, SLOTS + 2)):
            tile = act_ref[i // 2, :, i % 2 * WIDE + CH : i % 2 * WIDE + 2 * CH]
            transposed_row(tile, i, 0, lambda o: (o >= 0) & (o < length), act_t_ref)

    convolve(g_taps_ref, turned(w_ref), pair_ref, row_at, finish, beside)


def dpre2_kernel(
    len_ref, st_ref, hid_ref, back_ref, gain_ref, shift_ref, act_ref, dpre_ref, top_ref, bottom_ref, out_ref
):
    length = len_ref[0, 0]
    mean, inv = group_stats(st_ref)
    gain, shift = 0.5 * gain_ref[...], 0.5 * shift_ref[...]

    cross = plain = jnp.zeros((8, CH), F32)
    for r in range(SLOTS):
        normed = (hid_ref[r] - mean) * inv
        act, slope = silu_parts(normed * gain + shift)
        act_ref[r] = act.astype(BF16)
        grad = jnp.where(r < length, back_ref[r] * slope, 0.0)
        dpre_ref[r] = grad
        plain = plain + sums8(grad)
        cross = cross + sums8(grad * normed)
    send(out_ref, [jnp.sum(cross, axis=0, keepdims=True), jnp.sum(plain, axis=0, keepdims=True)])
    for ref, row in ((top_ref, 0), (bottom_ref, length - 1)):
        ref[0] = dpre_ref[row]
        ref[1] = hid_ref[row]


def grad2_kernel(len_ref, act_ref, g_taps_ref, out_ref, act_t_ref):
    length = len_ref[0, 0]
    half = SLOTS // 2
    for tap, o in ((0, 0), (0, 1), (1, 0), (1, SLOTS + 1), (2, SLOTS), (2, SLOTS + 1)):
        lanes = (o // 2 + 1) * COLS
        act_t_ref[o % 2, tap * CH : (tap + 1) * CH, lanes : lanes + COLS] = jnp.zeros((CH, COLS), BF16)
    for i in range(SLOTS):
        transposed_row(act_ref[i], i, 2, lambda o: i < length, act_t_ref)
    out_ref[...] = kernel_grad(
        act_t_ref, g_taps_ref[0 : half + 1, :, 0:WIDE], g_taps_ref[0 : half + 1, :, WIDE:PAIR]
    )


def dpre1_kernel(
    len_ref, st1_ref, st2_ref, sums_ref, own_sums_ref, hid_ref, dpre2_ref, up_ref, down_ref, act_t_ref,
    x_ref, grad2_ref, w_ref, gain1_ref, shift1_ref, gain2_ref,
    share_ref, dpre_ref, out_ref, d_taps_ref, grad1_ref, pair_ref,
):
    length, strip = len_ref[0, 0], lax.axis_index("strip")
    half = SLOTS // 2
    mean2, inv2 = group_stats(st2_ref)
    gain2 = gain2_ref[...]
    cross2, plain2 = moments(sums_ref, gain2)

    by_dpre, by_hidden, level = inv2 * gain2, inv2 * inv2 * cross2, inv2 * plain2

    def dhidden(dpre, hidden):
        return dpre * by_dpre - (hidden - mean2) * by_hidden - level

    mean1, inv1 = group_stats(st1_ref)
    gain1, shift1 = 0.5 * gain1_ref[...], 0.5 * shift1_ref[...]
    sums = [jnp.zeros((8, CH), F32), jnp.zeros((8, CH), F32)]

    def row_at(t):
        dpre = around(lambda r: dpre2_ref[r], up_ref[0], down_ref[0], length, t)
        hidden = around(lambda r: hid_ref[r], up_ref[1], down_ref[1], length, t)
        return jnp.where(in_image(length, strip, t), dhidden(dpre, hidden), 0.0)

    def finish(r, row):
        normed = (x_ref[r].astype(F32) - mean1) * inv1
        _, slope = silu_parts(normed * gain1 + shift1)
        grad = jnp.where(r < length, row * slope, 0.0)
        dpre_ref[r] = grad
        sums[0] = sums[0] + sums8(grad * normed)
        sums[1] = sums[1] + sums8(grad)

    convolve(d_taps_ref, turned(w_ref), pair_ref, row_at, finish, chunk=1)
    grad1_ref[...] = kernel_grad(act_t_ref, d_taps_ref[0:half, :, WIDE:PAIR], d_taps_ref[1 : half + 1, :, 0:WIDE])
    cross, plain = (jnp.sum(total, axis=0, keepdims=True) for total in sums)
    index = lax.broadcasted_iota(jnp.int32, (8, CH), 0)
    norm = jnp.where(index == 0, cross, jnp.where(index == 1, plain, 0.0))
    out_ref[...] = norm
    norm = norm + jnp.where(index == 2, own_sums_ref[0, 0:1], 0.0) + jnp.where(index == 3, own_sums_ref[0, 1:2], 0.0)
    blocks, rows = share_ref.shape[0], (share_ref.shape[1] - 8) // 2
    for j in range(blocks):
        share_ref[j] = packed(cut(grad1_ref, j * rows, rows), cut(grad2_ref, j * rows, rows), norm)


def cut(ref, begin, count):
    pieces = []
    while count:
        tap, row = divmod(begin, CH)
        here = min(count, CH - row)
        a, b = divmod(tap, 3)
        pieces.append(ref[a * CH + row : a * CH + row + here, (2 - b) * CH : (3 - b) * CH])
        begin, count = begin + here, count - here
    return pieces


def packed(first, second, norm):
    high = norm.astype(BF16).astype(F32)
    return jnp.concatenate([*first, *second, high[0:4], (norm - high)[0:4]], axis=0).astype(BF16)


def unpacked(total):
    rows = (total.shape[0] - 8) // 2
    norm = total[2 * rows : 2 * rows + 4] + total[2 * rows + 4 :]
    return total[0:rows], total[rows : 2 * rows], norm


def relay_kernel(in_ref, own_ref, out_ref):
    total = in_ref[0].astype(F32)
    for j in range(1, in_ref.shape[0]):
        total = total + in_ref[j].astype(F32)
    first, second, norm = unpacked(total)
    norm = jnp.concatenate([norm, jnp.zeros((4, CH), F32)], axis=0)
    own = own_ref[...]
    high = own.astype(BF16).astype(F32)
    image = jnp.concatenate([high[0:4], (own - high)[0:4]], axis=0).astype(BF16)
    tile = jnp.concatenate([packed([first], [second], norm), image], axis=0)
    for j in range(PEERS):
        out_ref[j] = tile


def finish_kernel(
    len_ref, in_ref, st_ref, x_ref, g_ref, dpre_ref, gain_ref, image_ref, first_ref, second_ref, norm_ref,
    rows_ref, first_own, second_own, norm_own, sem,
):
    total = in_ref[0].astype(F32)
    for j in range(1, PEERS):
        total = total + in_ref[j].astype(F32)
    rows = first_ref.shape[0]
    first_own[...], second_own[...], norm_own[...] = unpacked(total[0 : 2 * rows + 8])
    copies = []
    for k, (own, ref) in enumerate(((first_own, first_ref), (second_own, second_ref), (norm_own, norm_ref))):
        copies.append(pltpu.make_async_copy(own, ref, sem.at[STEPS + k]))
        copies[k].start()
    sums = total[2 * rows + 8 : 2 * rows + 12] + total[2 * rows + 12 : 2 * rows + 16]
    length = len_ref[0, 0]
    mean, inv = group_stats(st_ref)
    gain = gain_ref[...]
    cross, plain = folded(sums[0:1] * gain) / CELLS, folded(sums[1:2] * gain) / CELLS
    by_dpre, by_x, level = inv * gain, inv * inv * cross, inv * plain
    step = SLOTS // STEPS
    for k in range(STEPS):
        for r in range(k * step, (k + 1) * step):
            grad = dpre_ref[r] * by_dpre - (x_ref[r].astype(F32) - mean) * by_x - level
            rows_ref[r] = jnp.where(r < length, g_ref[r].astype(F32) + grad, 0.0).astype(BF16)
        part = pl.ds(k * step, step)
        copies.append(pltpu.make_async_copy(rows_ref.at[part], image_ref.at[part], sem.at[k]))
        copies[-1].start()
    for copy in copies:
        copy.wait()


def exchanged(value, axis):
    return lax.all_to_all(value, axis, split_axis=0, concat_axis=0, tiled=True)


def shifted(value, by):
    return lax.ppermute(value, "strip", [(i, (i + by) % PEERS) for i in range(PEERS)])


def body(
    image_in, cotangent, conv1_w, conv2_w, norm1_gain, norm1_shift, norm2_gain, norm2_shift, strip_rows
):
    x, g = image_in[0], cotangent[0]
    gain1, shift1 = norm1_gain[None], norm1_shift[None]
    gain2, shift2 = norm2_gain[None], norm2_shift[None]
    images = lax.axis_size(IMG)
    half = SLOTS // 2
    field = SLOTS * COLS * CH
    conv_flops = 2 * 9 * field * CH
    edge = (COLS, CH)
    stat = shape((PEERS, 8, CH), F32)

    ahead1, ahead2 = conv1_w.reshape(9 * CH, CH), conv2_w.reshape(9 * CH, CH)
    pair = pltpu.VMEM((2 * PAIR, 2 * CH), BF16)
    top, bottom, stats1 = call(
        stats_kernel,
        [SMEM] + [HBM] * 4,
        [shape((2, *edge), BF16), shape((2, *edge), BF16), stat],
        flops=field * 6,
        moved=field * 2,
        scratch=[
            pltpu.VMEM((SLOTS, *edge), BF16), pltpu.VMEM((1, CH), F32), pltpu.VMEM((1, CH), F32),
            pltpu.SemaphoreType.DMA((STEPS,)), pltpu.SemaphoreType.DMA((4,)), pltpu.SemaphoreType.DMA((2,)),
        ],
        limit=63 * MIB + MIB // 4,
    )(strip_rows, x, g, gain1, shift1)
    up, down = shifted(bottom, 1), shifted(top, -1)
    stats1 = exchanged(stats1, "strip")

    (act1,) = call(
        act1_kernel, [VMEM] * 2, [shape((half + 1, COLS, PAIR), BF16)], flops=field * 20, moved=field * 4
    )(x, stats1)
    hidden, act1, stats2 = call(
        hidden_kernel,
        [SMEM] + [VMEM] * 5,
        [shape((SLOTS, *edge), F32), shape((half + 1, COLS, PAIR), BF16), stat],
        flops=conv_flops,
        moved=field * 6,
        scratch=[pair],
        aliases={1: 1},
    )(strip_rows, act1, up, down, stats1, ahead1)

    g_taps, back2, act1_t = call(
        back_kernel,
        [SMEM] + [VMEM] * 5,
        [
            shape((half + 1, COLS, PAIR), BF16),
            shape((SLOTS, *edge), F32),
            shape((2, WIDE, (half + 2) * COLS), BF16),
        ],
        flops=conv_flops,
        moved=field * 6,
        scratch=[pair],
    )(strip_rows, g, up, down, ahead2, act1)
    stats2, g_taps, back2, act1_t = lax.optimization_barrier((stats2, g_taps, back2, act1_t))
    stats2 = exchanged(stats2, "strip")

    act2, dpre2, top, bottom, own_sums2 = call(
        dpre2_kernel,
        [SMEM] + [VMEM] * 5,
        [
            shape((SLOTS, *edge), BF16), shape((SLOTS, *edge), F32), shape((2, *edge), F32), shape((2, *edge), F32), stat,
        ],
        flops=field * 40,
        moved=field * 8,
    )(strip_rows, stats2, hidden, back2, gain2, shift2)
    up, down = shifted(bottom, 1), shifted(top, -1)

    (grad2,) = call(
        grad2_kernel,
        [SMEM] + [VMEM] * 2,
        [shape((WIDE, WIDE), F32)],
        flops=conv_flops,
        moved=field * 6,
        scratch=[pltpu.VMEM((2, WIDE, (half + 2) * COLS), BF16)],
    )(strip_rows, act2, g_taps)
    own_sums2, grad2 = lax.optimization_barrier((own_sums2, grad2))
    sums2 = exchanged(own_sums2, "strip")

    rows = 9 * CH // images
    share, dpre1, own_sums1 = call(
        dpre1_kernel,
        [SMEM] + [VMEM] * 15,
        [shape((images, 2 * rows + 8, CH), BF16), shape((SLOTS, *edge), F32), shape((8, CH), F32)],
        flops=2 * conv_flops,
        moved=field * 8,
        scratch=[pltpu.VMEM((half + 1, COLS, PAIR), BF16), pltpu.VMEM((WIDE, WIDE), F32), pair],
    )(
        strip_rows, stats1, stats2, sums2, own_sums2, hidden, dpre2, up, down, act1_t, x, grad2, ahead1,
        gain1, shift1, gain2,
    )
    share, dpre1, own_sums1 = lax.optimization_barrier((share, dpre1, own_sums1))
    share = exchanged(share, IMG)
    (relayed,) = call(
        relay_kernel, [VMEM, VMEM], [shape((PEERS, 2 * rows + 16, CH), BF16)], moved=images * (2 * rows + 8) * CH * 2
    )(share, own_sums1)
    relayed = exchanged(relayed, "strip")
    image_grad, grad1, grad2, norm_grads = call(
        finish_kernel,
        [SMEM] + [VMEM] * 6,
        [shape((SLOTS, *edge), BF16), shape((rows, CH), F32), shape((rows, CH), F32), shape((4, CH), F32)],
        flops=field * 12,
        moved=field * 10,
        scratch=[
            pltpu.VMEM((SLOTS, *edge), BF16), pltpu.VMEM((rows, CH), F32), pltpu.VMEM((rows, CH), F32),
            pltpu.VMEM((4, CH), F32), pltpu.SemaphoreType.DMA((STEPS + 3,)),
        ],
        outs_in=[HBM] * 4,
    )(strip_rows, relayed, stats1, x, g, dpre1, gain1)
    return image_grad[None], grad1, grad2, norm_grads


def solution(mesh):
    torus = Mesh(mesh.devices.reshape(4, 4, 2, mesh.shape["strip"]), (*IMG, "strip"))
    return jax.shard_map(
        body,
        mesh=torus,
        in_specs=(
            P(IMG, "strip", None, None), P(IMG, "strip", None, None), P(), P(), P(), P(), P(), P(), P(IMG, "strip"),
        ),
        out_specs=(P(IMG, "strip", None, None), P(IMG, None), P(IMG, None), P()),
        check_vma=False,
    )
```
